128 devices in a mesh: dp: 4 (over z), label: 32 (over y, x, core).
Axes of the slice: x: 4, y: 4, z: 4, core: 2. Of those that a mesh axis runs over, the one named last changes fastest.
Arguments:
- queries: bfloat16 [32768, 768], P(('dp', 'label')), may hold values from -6 to 6
- labels: bfloat16 [128, 512, 768], P('label'), may hold values from -0.21875 to 0.21875
- matcher: bfloat16 [128, 768], replicated, may hold values from -0.15 to 0.15
- cluster_ids: int32 [32768, 16], P('dp'), may hold values from 0 to 127, all different within a row; in each aligned block of 256 rows (0 to 255, 256 to 511, ...) at most 48 rows name the same one
- positives: int32 [32768], P('dp'), may hold values from 0 to 8191
Outputs:
- losses: float32 [32768], P(('dp', 'label'))
- query_grads: float32 [32768, 768], P(('dp', 'label'))
- label_grads: float32 [128, 512, 768], P('label', 'dp')
- matcher_grads: float32 [128, 768], replicated
The draws below stay inside these ranges and needn't reach their ends.
Inputs may be any that keep to these rules, and one draw needn't show every extreme that they name: `cluster_ids`: each row names 16 different leaf clusters; among the 256 rows of one device no cluster is named more than 48 times, and in every draw some device's rows name some cluster exactly 48 times.
All inputs are finite; a program needn't handle non-finite values.
Results may differ from the reference program's by a relative error of at most 0.0095.
Values may be sent and summed in bfloat16 or wider, within the bound.
A program may use at most 128 MiB of HBM per device.

```python
import math
import jax
import jax.numpy as jnp
import numpy as np
from jax import lax

D = 768
LEAF = 512
K = 16
Q_DEV = 256
QUERIES = 32768
CLUSTERS = 128
M = 48


def draw_queries(key, part):
    base_key = jax.random.fold_in(key, 11)
    rows = jnp.clip(jax.random.normal(base_key, (QUERIES, D), jnp.float32), -5.5, 5.5)
    return rows.astype(jnp.bfloat16)


def draw_matcher(key, part):
    root = (D * 1.0) ** 0.5
    noise = jax.random.normal(jax.random.fold_in(key, 21), (CLUSTERS, D), jnp.float32)
    noise = jnp.clip(noise, -4.0, 4.0) / root
    return jnp.clip(noise, -0.149, 0.149).astype(jnp.bfloat16)


def set_ends(entries, rng, low, largest):
    place = [jax.random.randint(jax.random.fold_in(rng, axis), (), 0, length) for axis, length in enumerate(entries.shape)]
    main_axis = entries.shape.index(max(entries.shape))
    neighbour = place[:main_axis] + [(place[main_axis] + 1) % entries.shape[main_axis]] + place[main_axis + 1:]
    return entries.at[tuple(place)].set(low).at[tuple(neighbour)].set(largest)


def steps_of(own_key, dims, shards, least, high):
    loudness, own = 1.0, jax.random.fold_in(own_key, 6)
    for axis_at, blocks in shards:
        draws = jnp.exp(jax.random.uniform(jax.random.fold_in(own, axis_at), (blocks,), jnp.float32, least / len(shards), high / len(shards)))
        loudness = loudness * jnp.repeat(draws, dims[axis_at] // blocks).reshape([-1 if axis == axis_at else 1 for axis in range(len(dims))])
    return loudness


def routed_block(stream_key, own, number, rows, amount, top, reach, slope):
    ranking = jax.random.permutation(stream_key, amount)
    heavy_load, common = shares(amount, rows * top, reach, slope, True), shares(amount, rows * top, reach, slope, False)
    places = jnp.arange(amount)

    def named(sizes, turn):
        used = int((sizes > 0).sum())
        fixed = max(1, used // 4)
        passed = fixed + (places - fixed + turn * (used - fixed)) % max(1, amount - fixed)
        return jnp.zeros((amount,), jnp.int32).at[ranking[jnp.where(places < fixed, places, passed)]].set(jnp.asarray(sizes, jnp.int32))

    sizes = jnp.where(number % 4 == 0, named(heavy_load, number // 4), named(common, number - number // 4 - 1))
    mixed = jax.random.permutation(jax.random.fold_in(own, 3), amount)
    donor, receiver = mixed[0:amount // 2 * 2:2], mixed[1:amount // 2 * 2:2]
    slack = jnp.minimum(sizes[donor] - 1, reach - sizes[receiver]) // 2
    slack = jnp.where((donor == ranking[0]) | (receiver == ranking[0]) | (sizes[receiver] == 0), 0, jnp.maximum(slack, 0))
    passed = jax.random.randint(jax.random.fold_in(own, 4), (amount // 2,), 0, 1 << 20) % (slack + 1)
    sizes = sizes.at[donor].add(-passed).at[receiver].add(passed)
    items = jnp.searchsorted(jnp.cumsum(sizes), jnp.arange(rows * top), side="right").astype(jnp.int32)
    grid = items.reshape(top, rows).T
    grid = grid[jax.random.permutation(jax.random.fold_in(own, 1), rows)]
    turn = jax.random.randint(jax.random.fold_in(own, 2), (rows, 1), 0, top)
    return jnp.take_along_axis(grid, (jnp.arange(top)[None, :] + turn) % top, axis=1)


def shares(amount, total, bound, skew, full):
    portions = [(1 << 20) // math.isqrt(rank ** skew) + 1 for rank in range(1, amount + 1)]
    largest = bound if full else min(bound, max(-(-total // amount), total * portions[0] // sum(portions)))
    least = 1 if total - largest >= amount - 1 else 0
    given, rest = [largest] + [least] * (amount - 1), total - largest - least * (amount - 1)
    while rest > 0:
        movable = [i for i in range(1, amount) if given[i] < largest] or [i for i in range(1, amount) if given[i] < bound]
        whole, left = sum([portions[i] for i in movable]), rest
        for i in movable:
            addition = min(bound - given[i], max(1, left * portions[i] // whole), rest)
            given[i] = given[i] + addition
            rest = rest - addition
    return np.array(given)


def normal_values(own_key, shape, width, bound, cuts=(), kind=jnp.bfloat16):
    drawn = width * jax.random.normal(own_key, shape, jnp.float32)
    if cuts:
        drawn = drawn * steps_of(own_key, shape, cuts, -0.22, 0.18)
    return jnp.clip(drawn, -bound, bound).astype(kind)


def setup_inputs(seed: int = 0) -> dict:
    streams_of = jax.random.split(jax.random.key(seed), 6)
    queries = draw_queries(jax.random.fold_in(streams_of[5], 71), 0)
    labels = normal_values(streams_of[1], (CLUSTERS, LEAF, D), D ** -0.5, 0.21875, ((0, 32),))
    matcher = draw_matcher(jax.random.fold_in(streams_of[5], 71), 0)
    cluster_ids_keys = jax.random.split(jax.random.fold_in(streams_of[3], 1), QUERIES // Q_DEV)
    cluster_ids_turns = jax.random.permutation(jax.random.fold_in(streams_of[3], 3), QUERIES // Q_DEV)
    cluster_ids = jax.vmap(lambda own, number: routed_block(jax.random.fold_in(streams_of[3], 2), own, number, Q_DEV, CLUSTERS, K, M, 1))(cluster_ids_keys, cluster_ids_turns).reshape((QUERIES, K))
    positives = set_ends(jax.random.randint(streams_of[4], (QUERIES,), 0, K * LEAF), jax.random.fold_in(streams_of[4], 1), 0, (K * LEAF) - 1).astype(jnp.int32)
    return dict(queries=queries, labels=labels, matcher=matcher, cluster_ids=cluster_ids, positives=positives)


BIG = 1.0e30


def block_ranks(block_ids):
    flat = block_ids.reshape(-1)
    onehot = (flat[:, None] == jnp.arange(CLUSTERS, dtype=jnp.int32)[None, :]).astype(jnp.int32)
    running = jnp.cumsum(onehot, axis=0) - 1
    return jnp.sum(running * onehot, axis=1).astype(jnp.int32)


def reference(queries, labels, matcher, cluster_ids, positives):
    n_blocks = QUERIES // Q_DEV
    span = n_blocks * M
    ranks = lax.map(block_ranks, cluster_ids.reshape(n_blocks, Q_DEV * K))
    entry = jnp.arange(QUERIES * K, dtype=jnp.int32)
    row = entry // K
    slot_k = entry % K
    flat_ids = cluster_ids.reshape(-1).astype(jnp.int32)
    flat_rank = ranks.reshape(-1).astype(jnp.int32)
    block = row // Q_DEV
    flat_pos = positives[row]
    target = jnp.where(flat_pos // LEAF == slot_k, flat_pos % LEAF, -1).astype(jnp.int32)
    row_map = jnp.full((CLUSTERS, n_blocks, M), QUERIES, jnp.int32).at[flat_ids, block, flat_rank].set(row)
    target_map = jnp.full((CLUSTERS, n_blocks, M), -1, jnp.int32).at[flat_ids, block, flat_rank].set(target)
    row_map = row_map.reshape(CLUSTERS, span)
    target_map = target_map.reshape(CLUSTERS, span)
    queries_f = queries.astype(jnp.float32)
    leaf_iota = jnp.arange(LEAF, dtype=jnp.int32)
    hp = lax.Precision.HIGHEST

    def cluster_scores(index):
        rows = queries_f[jnp.minimum(row_map[index], QUERIES - 1)]
        weights = labels[index].astype(jnp.float32)
        match = matcher[index].astype(jnp.float32)
        scores = jnp.dot(rows, weights.T, precision=hp) + jnp.dot(rows, match, precision=hp)[:, None]
        hit = (leaf_iota[None, :] == target_map[index][:, None]).astype(jnp.float32)
        return rows, weights, match, scores, hit

    def first_pass(index):
        rows, weights, match, scores, hit = cluster_scores(index)
        top = jnp.max(scores, axis=1)
        total = jnp.sum(jnp.exp(scores - top[:, None]), axis=1)
        return top, total, jnp.sum(scores * hit, axis=1)

    tops, totals, picked = lax.map(first_pass, jnp.arange(CLUSTERS, dtype=jnp.int32))
    where = flat_ids * span + block * M + flat_rank
    slot_top = tops.reshape(-1)[where].reshape(QUERIES, K)
    slot_total = totals.reshape(-1)[where].reshape(QUERIES, K)
    slot_picked = picked.reshape(-1)[where].reshape(QUERIES, K)
    best = jnp.max(slot_top, axis=1)
    lse = best + jnp.log(jnp.sum(slot_total * jnp.exp(slot_top - best[:, None]), axis=1))
    losses = lse - jnp.sum(slot_picked, axis=1)
    slot_lse = jnp.where(row_map < QUERIES, lse[jnp.minimum(row_map, QUERIES - 1)], BIG)

    def second_pass(carry, index):
        rows, weights, match, scores, hit = cluster_scores(index)
        delta = jnp.exp(scores - slot_lse[index][:, None]) - hit
        coef = jnp.sum(delta, axis=1)
        delta_b = lax.optimization_barrier(delta.astype(jnp.bfloat16)).astype(jnp.float32)
        coef_b = lax.optimization_barrier(coef.astype(jnp.bfloat16)).astype(jnp.float32)
        slot_grad = jnp.dot(delta_b, weights, precision=hp) + coef_b[:, None] * match[None, :]
        slot_grad = lax.optimization_barrier(slot_grad.astype(jnp.bfloat16)).astype(jnp.float32)
        label_grad = jnp.dot(delta_b.T, rows, precision=hp)
        matcher_grad = jnp.dot(coef_b, rows, precision=hp)
        carry = carry.at[row_map[index]].add(slot_grad, mode="drop")
        return carry, (label_grad, matcher_grad)

    start = jnp.zeros((QUERIES, D), jnp.float32)
    query_grads, stacked = lax.scan(second_pass, start, jnp.arange(CLUSTERS, dtype=jnp.int32))
    return losses, query_grads, stacked[0], stacked[1]
```

```python
import jax
import jax.numpy as jnp
from jax import lax
from jax.sharding import PartitionSpec as P

LEAF = 512
K = 16


BIG = 1e30


def in_one_piece(arrays, axis, split_dim, concat_dim, along):
    widths = [a.shape[along] for a in arrays]
    both = jnp.concatenate(arrays, axis=along)
    filled = lax.all_to_all(both, axis, split_axis=split_dim, concat_axis=concat_dim, tiled=True)
    return tuple(jnp.split(filled, [sum(widths[:k]) for k in range(1, len(widths))], axis=along))


def sent_to_all(shard, axis):
    devices = lax.axis_size(axis)
    return lax.all_to_all(
        jnp.broadcast_to(shard[None], (devices, *shard.shape)), axis, 0, 0, tiled=True
    )


def over_copies(shard, axis):
    return sent_to_all(shard, axis).sum(axis=0)


def earlier_counts(named):
    count = named.shape[-2]
    iota = jnp.arange(count, dtype=jnp.int32)
    lower = (iota[:, None] > iota[None, :]).astype(jnp.bfloat16)
    return jnp.einsum(
        "ij,sjc->sic", lower, named.astype(jnp.bfloat16), preferred_element_type=jnp.float32
    )


def body(queries, labels, matcher, cluster_ids, positives):
    q_dev, width = queries.shape
    cl_dev = labels.shape[0]
    clusters = matcher.shape[0]
    n_label = lax.axis_size("label")
    capacity = q_dev * K * 3 // (2 * clusters)
    rows_dev = n_label * capacity
    me = lax.axis_index("label")
    first = me * cl_dev
    slot_iota = jnp.arange(capacity, dtype=jnp.float32)
    shortlist_iota = jnp.arange(K, dtype=jnp.int32)
    own_ids = lax.dynamic_slice_in_dim(cluster_ids, me * q_dev, q_dev, 0)
    all_iota = jnp.arange(clusters, dtype=jnp.int32)
    named_own = jnp.any(own_ids[:, :, None] == all_iota[None, None, :], axis=1)
    rank_own = earlier_counts(named_own[None])[0]
    select_own = named_own.T[:, None, :] & (rank_own.T[:, None, :] == slot_iota[None, :, None])
    select_own = select_own.reshape(n_label, cl_dev, capacity, q_dev).transpose(1, 0, 2, 3)
    group_ids = cluster_ids.reshape(n_label, q_dev, K) - first
    group_pos = positives.reshape(n_label, q_dev)
    local_iota = jnp.arange(cl_dev, dtype=jnp.int32)
    named_recv = jnp.any(group_ids[:, :, :, None] == local_iota[None, None, None, :], axis=2)
    rank_recv = earlier_counts(named_recv)
    named_t = named_recv.transpose(2, 0, 1)
    rank_t = rank_recv.transpose(2, 0, 1)
    select_recv = named_t[:, :, None, :] & (rank_t[:, :, None, :] == slot_iota[None, None, :, None])
    pos_slot = group_pos // LEAF
    pos_cluster = jnp.sum(
        jnp.where(shortlist_iota[None, None, :] == pos_slot[:, :, None], group_ids, 0), axis=2
    )
    target_val = jnp.where(
        pos_cluster[None, :, :] == local_iota[:, None, None], (group_pos % LEAF)[None, :, :], -1
    )
    target_map = jnp.sum(jnp.where(select_recv, target_val[:, :, None, :] + 1, 0), axis=3) - 1
    group = lax.all_gather(queries, "label", axis=0, tiled=True).reshape(n_label, q_dev, width)
    picked_rows = jnp.einsum(
        "csri,sid->csrd",
        select_recv.astype(jnp.bfloat16),
        group,
        preferred_element_type=jnp.float32,
    )
    received = picked_rows.astype(jnp.bfloat16).reshape(cl_dev, rows_dev, width)
    match_own = lax.dynamic_slice_in_dim(matcher, first, cl_dev, 0)
    scores = jnp.einsum("csd,cld->csl", received, labels, preferred_element_type=jnp.float32)
    bias = jnp.einsum("csd,cd->cs", received, match_own, preferred_element_type=jnp.float32)
    scores = scores + bias[:, :, None]
    leaf_iota = jnp.arange(LEAF, dtype=jnp.int32)
    hit = (leaf_iota[None, None, :] == target_map.reshape(cl_dev, rows_dev)[:, :, None]).astype(
        jnp.float32
    )
    top = jnp.max(scores, axis=2)
    total = jnp.sum(jnp.exp(scores - top[:, :, None]), axis=2)
    picked = jnp.sum(scores * hit, axis=2)
    shape3 = (cl_dev, n_label, capacity)
    back_top, back_total, back_picked = in_one_piece(
        (top.reshape(shape3), total.reshape(shape3), picked.reshape(shape3)), "label", 1, 1, 0
    )
    best = jnp.max(jnp.where(select_own, back_top[..., None], -BIG), axis=(0, 1, 2))
    spread = jnp.where(
        select_own,
        back_total[..., None] * jnp.exp(back_top[..., None] - best[None, None, None, :]),
        0.0,
    )
    lse = best + jnp.log(jnp.sum(spread, axis=(0, 1, 2)))
    losses = lse - jnp.sum(jnp.where(select_own, back_picked[..., None], 0.0), axis=(0, 1, 2))
    used = jnp.any(select_own, axis=3)
    outgoing_lse = jnp.where(
        used, jnp.sum(jnp.where(select_own, lse[None, None, None, :], 0.0), axis=3), BIG
    )
    slot_lse = lax.all_to_all(
        outgoing_lse, "label", split_axis=1, concat_axis=1, tiled=True
    ).reshape(cl_dev, rows_dev)
    delta = jnp.exp(scores - slot_lse[:, :, None]) - hit
    coef = jnp.sum(delta, axis=2)
    delta_b = delta.astype(jnp.bfloat16)
    coef_b = coef.astype(jnp.bfloat16)
    slot_grad = jnp.einsum("csl,cld->csd", delta_b, labels, preferred_element_type=jnp.float32)
    slot_grad = (
        slot_grad
        + coef_b.astype(jnp.float32)[:, :, None] * match_own.astype(jnp.float32)[:, None, :]
    )
    slot_grad = slot_grad.astype(jnp.bfloat16).reshape(cl_dev, n_label, capacity, width)
    partial = jnp.einsum(
        "csri,csrd->sid",
        select_recv.astype(jnp.bfloat16),
        slot_grad,
        preferred_element_type=jnp.float32,
    )
    query_grads = lax.psum_scatter(
        partial.astype(jnp.bfloat16).reshape(n_label * q_dev, width),
        "label",
        scatter_dimension=0,
        tiled=True,
    ).astype(jnp.float32)
    label_part = jnp.einsum("csl,csd->cld", delta_b, received, preferred_element_type=jnp.float32)
    label_grads = lax.psum_scatter(
        label_part.astype(jnp.bfloat16), "dp", scatter_dimension=1, tiled=True
    ).astype(jnp.float32)
    local_sum = jnp.einsum("cs,csd->cd", coef_b, received, preferred_element_type=jnp.float32)
    local_sum = over_copies(local_sum, "dp")
    matcher_grads = lax.all_gather(local_sum, "label", axis=0, tiled=True)
    return (losses, query_grads, label_grads, matcher_grads)


def solution(mesh):
    return jax.shard_map(
        body,
        mesh=mesh,
        in_specs=(P(("dp", "label"), None), P("label", None, None), P(), P("dp", None), P("dp")),
        out_specs=(P(("dp", "label")), P(("dp", "label"), None), P("label", "dp", None), P()),
        check_vma=False,
    )
```

```python
import jax
import jax.numpy as jnp
from jax import lax
from jax.experimental import pallas as pl
from jax.experimental.pallas import tpu as pltpu
from jax.sharding import PartitionSpec as P

LEAF = 512
K = 16


BIG = 1e30


def in_one_piece(arrays, axis, split_dim, concat_dim, along):
    widths = [a.shape[along] for a in arrays]
    both = jnp.concatenate(arrays, axis=along)
    filled = lax.all_to_all(both, axis, split_axis=split_dim, concat_axis=concat_dim, tiled=True)
    return tuple(jnp.split(filled, [sum(widths[:k]) for k in range(1, len(widths))], axis=along))


def sent_to_all(shard, axis):
    devices = lax.axis_size(axis)
    return lax.all_to_all(
        jnp.broadcast_to(shard[None], (devices, *shard.shape)), axis, 0, 0, tiled=True
    )


def over_copies(shard, axis):
    return sent_to_all(shard, axis).sum(axis=0)


def earlier_counts(named):
    count = named.shape[-2]
    iota = jnp.arange(count, dtype=jnp.int32)
    lower = (iota[:, None] > iota[None, :]).astype(jnp.bfloat16)
    return jnp.einsum(
        "ij,sjc->sic", lower, named.astype(jnp.bfloat16), preferred_element_type=jnp.float32
    )


MESH = pl.DeviceIdType.MESH

def place():
    me = lax.axis_index("label")
    core = lax.rem(me, 2)
    x = lax.rem(me // 2, 4)
    y = me // 8
    a = x * (1 - core) + y * core
    b = y * (1 - core) + x * core
    return me, core, a, b

def index_of(core, a, b):
    x = a * (1 - core) + b * core
    y = b * (1 - core) + a * core
    return (y * 4 + x) * 2 + core

OFF = (0, 3, 1, 2)

class Links:
    def __init__(self, send, recv):
        self.me, self.core, self.a, self.b = place()
        self.send, self.recv, self.sent = send, recv, []
        c, a, b = self.core, self.a, self.b
        self.partner = self.me + 1 - 2 * c
        self.dev = {
            "a-": index_of(c, lax.rem(a + 3, 4), b),
            "a+": index_of(c, lax.rem(a + 1, 4), b),
            "b-": index_of(c, a, lax.rem(b + 3, 4)),
            "b+": index_of(c, a, lax.rem(b + 1, 4)),
            "p": self.partner,
        }
    def block(self, i, j):
        return index_of(self.core, lax.rem(self.a + OFF[i], 4), lax.rem(self.b + OFF[j], 4))
    def partner_block(self, i, j):
        return index_of(1 - self.core, lax.rem(self.b + OFF[i], 4), lax.rem(self.a + OFF[j], 4))
    def meet(self):
        barrier = pltpu.get_barrier_semaphore()
        for d in self.dev.values():
            pl.semaphore_signal(barrier, inc=1, device_id={"label": d}, device_id_type=MESH)
        pl.semaphore_wait(barrier, 5)
    def copy(self, src, dst, slot, to):
        n = len(self.sent)
        c = pltpu.make_async_remote_copy(src_ref=src, dst_ref=dst, send_sem=self.send.at[n],
            recv_sem=self.recv.at[slot], device_id={"label": self.dev[to]}, device_id_type=MESH)
        c.start()
        self.sent.append(c)
    def wait(self, dst, slot):
        pltpu.make_async_remote_copy(src_ref=dst, dst_ref=dst, send_sem=self.send.at[0],
            recv_sem=self.recv.at[slot], device_id={"label": self.partner}, device_id_type=MESH).wait_recv()
    def drain(self):
        for c in self.sent:
            c.wait_send()

def gather_kernel(q_ref, g, send, recv):
    L = Links(send, recv)
    L.meet()
    half = q_ref.shape[0] // 2
    lo = lambda k: g.at[k, pl.ds(0, half)]
    hi = lambda k: g.at[k, pl.ds(half, half)]
    own = L.block(0, 0)
    for to, slot in (("a+", 0), ("a-", 1), ("b+", 4), ("b-", 5), ("p", 20)):
        L.copy(q_ref, g.at[own], slot, to)
    g[own] = q_ref[...]
    def side_a(i):
        k = L.block(i, 0)
        L.wait(g.at[k], i - 1)
        if i == 1:
            L.copy(lo(k), lo(k), 2, "a+")
        else:
            L.copy(hi(k), hi(k), 3, "a-")
        L.copy(g.at[k], g.at[k], 4 + 4 * i, "b+")
        L.copy(g.at[k], g.at[k], 5 + 4 * i, "b-")
        L.copy(g.at[k], g.at[k], 20 + 4 * i, "p")
    def far_a():
        k = L.block(3, 0)
        L.wait(lo(k), 2)
        L.wait(hi(k), 3)
        L.copy(g.at[k], g.at[k], 16, "b+")
        L.copy(g.at[k], g.at[k], 17, "b-")
        L.copy(g.at[k], g.at[k], 32, "p")
    def side_b(i):
        k = L.block(i, 1)
        L.wait(g.at[k], 4 + 4 * i)
        L.copy(lo(k), lo(k), 6 + 4 * i, "b+")
        L.copy(g.at[k], g.at[k], 21 + 4 * i, "p")
        k = L.block(i, 2)
        L.wait(g.at[k], 5 + 4 * i)
        L.copy(hi(k), hi(k), 7 + 4 * i, "b-")
        L.copy(g.at[k], g.at[k], 22 + 4 * i, "p")
    def far_b(i):
        k = L.block(i, 3)
        L.wait(lo(k), 6 + 4 * i)
        L.wait(hi(k), 7 + 4 * i)
        L.copy(g.at[k], g.at[k], 23 + 4 * i, "p")
    def from_partner(i, j):
        k = L.partner_block(i, j)
        L.wait(g.at[k], 20 + 4 * i + j)
    side_a(1); side_a(2); side_b(0); far_a(); side_b(1); far_b(0); side_b(2); far_b(1); side_b(3); far_b(2); far_b(3)
    for i in range(4):
        for j in range(4):
            from_partner(i, j)
    L.drain()

def gather(q):
    return pl.pallas_call(
        gather_kernel,
        out_shape=jax.ShapeDtypeStruct((32, *q.shape), q.dtype),
        in_specs=[pl.BlockSpec(memory_space=pltpu.VMEM)],
        out_specs=pl.BlockSpec(memory_space=pltpu.VMEM),
        scratch_shapes=[pltpu.SemaphoreType.DMA((36,)), pltpu.SemaphoreType.DMA((36,))],
        compiler_params=pltpu.CompilerParams(collective_id=0, has_side_effects=True),
    )(q)

def scatter_kernel(p, out, t, u, pr, bh, bf, ah, af, send, recv):
    L = Links(send, recv)
    L.meet()
    half = p.shape[1] // 2
    f32 = jnp.float32
    ORDER = [(i, 3) for i in (3, 1, 2, 0)] + [(i, j) for i in (3, 1, 2, 0) for j in (1, 2)] + [(i, 0) for i in (3, 1, 2, 0)]
    for i, j in ORDER:
        L.copy(p.at[L.partner_block(i, j)], pr.at[4 * i + j], 4 * i + j, "p")
    LO, HI = pl.ds(0, half), pl.ds(half, half)
    def both(i, j):
        L.wait(pr.at[4 * i + j], 4 * i + j)
        return lambda s: p[L.block(i, j), s].astype(f32) + pr[4 * i + j, s].astype(f32)
    for i in (3, 1, 2, 0):
        s = both(i, 3)
        n = 3 * i + 2
        t[n] = s(slice(None)).astype(t.dtype)
        L.copy(t.at[n, LO], bh.at[i, 0], 16 + 4 * i, "b+")
        L.copy(t.at[n, HI], bh.at[i, 1], 17 + 4 * i, "b-")
    for i in (3, 1, 2, 0):
        s = both(i, 2)
        n = 3 * i + 1
        L.wait(bh.at[i, 0], 16 + 4 * i)
        t[n, LO] = (s(LO) + bh[i, 0].astype(f32)).astype(t.dtype)
        t[n, HI] = s(HI).astype(t.dtype)
        L.copy(t.at[n], bf.at[i, 0], 18 + 4 * i, "b+")
        s = both(i, 1)
        n = 3 * i
        L.wait(bh.at[i, 1], 17 + 4 * i)
        t[n, HI] = (s(HI) + bh[i, 1].astype(f32)).astype(t.dtype)
        t[n, LO] = s(LO).astype(t.dtype)
        L.copy(t.at[n], bf.at[i, 1], 19 + 4 * i, "b-")
    def column(i):
        s = both(i, 0)
        L.wait(bf.at[i, 0], 18 + 4 * i)
        L.wait(bf.at[i, 1], 19 + 4 * i)
        return lambda r: s(r) + bf[i, 0, r].astype(f32) + bf[i, 1, r].astype(f32)
    s = column(3)
    u[2] = s(slice(None)).astype(u.dtype)
    L.copy(u.at[2, LO], ah.at[0], 32, "a+")
    L.copy(u.at[2, HI], ah.at[1], 33, "a-")
    s = column(1)
    L.wait(ah.at[1], 33)
    u[0, HI] = (s(HI) + ah[1].astype(f32)).astype(u.dtype)
    u[0, LO] = s(LO).astype(u.dtype)
    L.copy(u.at[0], af.at[1], 35, "a-")
    s = column(2)
    L.wait(ah.at[0], 32)
    u[1, LO] = (s(LO) + ah[0].astype(f32)).astype(u.dtype)
    u[1, HI] = s(HI).astype(u.dtype)
    L.copy(u.at[1], af.at[0], 34, "a+")
    s = column(0)
    L.wait(af.at[0], 34)
    L.wait(af.at[1], 35)
    out[...] = s(slice(None)) + af[0].astype(f32) + af[1].astype(f32)
    L.drain()

def scatter(p):
    n, r, w = p.shape
    bf16 = jnp.bfloat16
    return pl.pallas_call(
        scatter_kernel,
        out_shape=jax.ShapeDtypeStruct((r, w), jnp.float32),
        in_specs=[pl.BlockSpec(memory_space=pltpu.VMEM)],
        out_specs=pl.BlockSpec(memory_space=pltpu.VMEM),
        scratch_shapes=[pltpu.VMEM((12, r, w), bf16), pltpu.VMEM((3, r, w), bf16), pltpu.VMEM((16, r, w), bf16),
            pltpu.VMEM((4, 2, r // 2, w), bf16), pltpu.VMEM((4, 2, r, w), bf16), pltpu.VMEM((2, r // 2, w), bf16), pltpu.VMEM((2, r, w), bf16),
            pltpu.SemaphoreType.DMA((36,)), pltpu.SemaphoreType.DMA((36,))],
        compiler_params=pltpu.CompilerParams(collective_id=1, has_side_effects=True),
    )(p)


def body(queries, labels, matcher, cluster_ids, positives):
    q_dev, width = queries.shape
    cl_dev = labels.shape[0]
    clusters = matcher.shape[0]
    n_label = lax.axis_size("label")
    capacity = q_dev * K * 3 // (2 * clusters)
    rows_dev = n_label * capacity
    me = lax.axis_index("label")
    first = me * cl_dev
    slot_iota = jnp.arange(capacity, dtype=jnp.float32)
    shortlist_iota = jnp.arange(K, dtype=jnp.int32)
    own_ids = lax.dynamic_slice_in_dim(cluster_ids, me * q_dev, q_dev, 0)
    all_iota = jnp.arange(clusters, dtype=jnp.int32)
    named_own = jnp.any(own_ids[:, :, None] == all_iota[None, None, :], axis=1)
    rank_own = earlier_counts(named_own[None])[0]
    select_own = named_own.T[:, None, :] & (rank_own.T[:, None, :] == slot_iota[None, :, None])
    select_own = select_own.reshape(n_label, cl_dev, capacity, q_dev).transpose(1, 0, 2, 3)
    group_ids = cluster_ids.reshape(n_label, q_dev, K) - first
    group_pos = positives.reshape(n_label, q_dev)
    local_iota = jnp.arange(cl_dev, dtype=jnp.int32)
    named_recv = jnp.any(group_ids[:, :, :, None] == local_iota[None, None, None, :], axis=2)
    rank_recv = earlier_counts(named_recv)
    named_t = named_recv.transpose(2, 0, 1)
    rank_t = rank_recv.transpose(2, 0, 1)
    select_recv = named_t[:, :, None, :] & (rank_t[:, :, None, :] == slot_iota[None, None, :, None])
    pos_slot = group_pos // LEAF
    pos_cluster = jnp.sum(
        jnp.where(shortlist_iota[None, None, :] == pos_slot[:, :, None], group_ids, 0), axis=2
    )
    target_val = jnp.where(
        pos_cluster[None, :, :] == local_iota[:, None, None], (group_pos % LEAF)[None, :, :], -1
    )
    target_map = jnp.sum(jnp.where(select_recv, target_val[:, :, None, :] + 1, 0), axis=3) - 1
    group = gather(queries)
    picked_rows = jnp.einsum(
        "csri,sid->csrd",
        select_recv.astype(jnp.bfloat16),
        group,
        preferred_element_type=jnp.float32,
    )
    received = picked_rows.astype(jnp.bfloat16).reshape(cl_dev, rows_dev, width)
    match_own = lax.dynamic_slice_in_dim(matcher, first, cl_dev, 0)
    scores = jnp.einsum("csd,cld->csl", received, labels, preferred_element_type=jnp.float32)
    bias = jnp.einsum("csd,cd->cs", received, match_own, preferred_element_type=jnp.float32)
    scores = scores + bias[:, :, None]
    leaf_iota = jnp.arange(LEAF, dtype=jnp.int32)
    hit = (leaf_iota[None, None, :] == target_map.reshape(cl_dev, rows_dev)[:, :, None]).astype(
        jnp.float32
    )
    top = jnp.max(scores, axis=2)
    total = jnp.sum(jnp.exp(scores - top[:, :, None]), axis=2)
    picked = jnp.sum(scores * hit, axis=2)
    shape3 = (cl_dev, n_label, capacity)
    back_top, back_total, back_picked = in_one_piece(
        (top.reshape(shape3), total.reshape(shape3), picked.reshape(shape3)), "label", 1, 1, 0
    )
    best = jnp.max(jnp.where(select_own, back_top[..., None], -BIG), axis=(0, 1, 2))
    spread = jnp.where(
        select_own,
        back_total[..., None] * jnp.exp(back_top[..., None] - best[None, None, None, :]),
        0.0,
    )
    lse = best + jnp.log(jnp.sum(spread, axis=(0, 1, 2)))
    losses = lse - jnp.sum(jnp.where(select_own, back_picked[..., None], 0.0), axis=(0, 1, 2))
    used = jnp.any(select_own, axis=3)
    outgoing_lse = jnp.where(
        used, jnp.sum(jnp.where(select_own, lse[None, None, None, :], 0.0), axis=3), BIG
    )
    slot_lse = lax.all_to_all(
        outgoing_lse, "label", split_axis=1, concat_axis=1, tiled=True
    ).reshape(cl_dev, rows_dev)
    delta = jnp.exp(scores - slot_lse[:, :, None]) - hit
    coef = jnp.sum(delta, axis=2)
    delta_b = delta.astype(jnp.bfloat16)
    coef_b = coef.astype(jnp.bfloat16)
    slot_grad = jnp.einsum("csl,cld->csd", delta_b, labels, preferred_element_type=jnp.float32)
    slot_grad = (
        slot_grad
        + coef_b.astype(jnp.float32)[:, :, None] * match_own.astype(jnp.float32)[:, None, :]
    )
    slot_grad = slot_grad.astype(jnp.bfloat16).reshape(cl_dev, n_label, capacity, width)
    partial = jnp.einsum(
        "csri,csrd->sid",
        select_recv.astype(jnp.bfloat16),
        slot_grad,
        preferred_element_type=jnp.float32,
    )
    query_grads = scatter(partial.astype(jnp.bfloat16))
    label_part = jnp.einsum("csl,csd->cld", delta_b, received, preferred_element_type=jnp.float32)
    label_grads = lax.psum_scatter(
        label_part.astype(jnp.bfloat16), "dp", scatter_dimension=1, tiled=True
    ).astype(jnp.float32)
    local_sum = jnp.einsum("cs,csd->cd", coef_b, received, preferred_element_type=jnp.float32)
    local_sum = over_copies(local_sum, "dp")
    matcher_grads = lax.all_gather(local_sum, "label", axis=0, tiled=True)
    return (losses, query_grads, label_grads, matcher_grads)


def solution(mesh):
    return jax.shard_map(
        body,
        mesh=mesh,
        in_specs=(P(("dp", "label"), None), P("label", None, None), P(), P("dp", None), P("dp")),
        out_specs=(P(("dp", "label")), P(("dp", "label"), None), P("label", "dp", None), P()),
        check_vma=False,
    )
```

```python
import jax
import jax.numpy as jnp
from jax import lax
from jax.experimental import pallas as pl
from jax.experimental.pallas import tpu as pltpu
from jax.sharding import PartitionSpec as P

LEAF = 512
K = 16
BIG = 1e30

MESH = pl.DeviceIdType.MESH

def place():
    me = lax.axis_index("label")
    core = lax.rem(me, 2)
    x = lax.rem(me // 2, 4)
    y = me // 8
    a = x * (1 - core) + y * core
    b = y * (1 - core) + x * core
    return me, core, a, b

def index_of(core, a, b):
    x = a * (1 - core) + b * core
    y = b * (1 - core) + a * core
    return (y * 4 + x) * 2 + core

OFF = (0, 3, 1, 2)

class Links:
    def __init__(self, send, recv):
        self.me, self.core, self.a, self.b = place()
        self.send, self.recv, self.sent = send, recv, []
        c, a, b = self.core, self.a, self.b
        self.partner = self.me + 1 - 2 * c
        self.dev = {
            "a-": index_of(c, lax.rem(a + 3, 4), b),
            "a+": index_of(c, lax.rem(a + 1, 4), b),
            "b-": index_of(c, a, lax.rem(b + 3, 4)),
            "b+": index_of(c, a, lax.rem(b + 1, 4)),
            "p": self.partner,
        }
    def block(self, i, j):
        return index_of(self.core, lax.rem(self.a + OFF[i], 4), lax.rem(self.b + OFF[j], 4))
    def partner_block(self, i, j):
        return index_of(1 - self.core, lax.rem(self.b + OFF[i], 4), lax.rem(self.a + OFF[j], 4))
    def meet(self, peers=None):
        barrier = pltpu.get_barrier_semaphore()
        peers = list(self.dev.values()) if peers is None else peers
        for d in peers:
            pl.semaphore_signal(barrier, inc=1, device_id={"label": d}, device_id_type=MESH)
        pl.semaphore_wait(barrier, len(peers))
    def copy(self, src, dst, slot, to):
        n = len(self.sent)
        c = pltpu.make_async_remote_copy(src_ref=src, dst_ref=dst, send_sem=self.send.at[n],
            recv_sem=self.recv.at[slot], device_id={"label": self.dev[to]}, device_id_type=MESH)
        c.start()
        self.sent.append(c)
    def wait(self, dst, slot):
        pltpu.make_async_remote_copy(src_ref=dst, dst_ref=dst, send_sem=self.send.at[0],
            recv_sem=self.recv.at[slot], device_id={"label": self.partner}, device_id_type=MESH).wait_recv()
    def drain(self):
        for c in self.sent:
            c.wait_send()


SLOTS = 48


def slot_tables(ids, pos):
    f32 = jnp.float32
    n = ids.shape[1]
    rows = lax.broadcasted_iota(jnp.int32, ids.shape, 0)
    pos_cluster = jnp.sum(
        jnp.where(rows == (pos >> 9), ids, 0).astype(f32), axis=0, keepdims=True
    )
    line = lax.broadcasted_iota(jnp.int32, (8, n), 0)
    named = jnp.zeros((8, n), f32)
    for c in range(4):
        hit = jnp.sum((ids == c).astype(f32), axis=0, keepdims=True)
        named = jnp.where(line == c, hit, named)
    earlier = (
        lax.broadcasted_iota(jnp.int32, (n, n), 0) < lax.broadcasted_iota(jnp.int32, (n, n), 1)
    ).astype(f32)
    rank = jnp.dot(
        named.astype(jnp.bfloat16), earlier.astype(jnp.bfloat16), preferred_element_type=f32
    )
    code = jnp.where(named > 0.5, rank, -1.0)
    target = ((pos & (LEAF - 1)) + 1).astype(f32)
    targets = jnp.where(pos_cluster == (line - 4).astype(f32), target, 0.0)
    return jnp.where(line < 4, code, targets)


def picks(info, c):
    r = lax.broadcasted_iota(jnp.int32, (SLOTS, info.shape[1]), 0).astype(jnp.float32)
    return info[c : c + 1] == r


def target_column(info, pick, c):
    return jnp.sum(jnp.where(pick, info[4 + c : 5 + c], 0.0), axis=1, keepdims=True) - 1.0


def forward_kernel(q_ref, labels, match, ids_ref, pos_ref, scores_out, rec_out, info, lse, losses,
                   g, scores, rec, st, sr, send, recv, st_send, st_recv, lse_send, lse_recv, out_sem):
    f32 = jnp.float32
    L = Links(send, recv)
    peers = [(k, L.block(i, j)) for k, (i, j) in enumerate([(i, j) for i in range(4) for j in range(4)])]
    peers = [d for k, d in peers if k > 0]
    peers += [L.partner_block(i, j) for i in range(4) for j in range(4)]
    L.meet(peers)
    half = q_ref.shape[0] // 2
    first = L.me * 4
    lo = lambda k: g.at[k, pl.ds(0, half)]
    hi = lambda k: g.at[k, pl.ds(half, half)]
    own = L.block(0, 0)
    for to, slot in (("a+", 0), ("a-", 1), ("b+", 4), ("b-", 5), ("p", 20)):
        L.copy(q_ref, g.at[own], slot, to)
    g[own] = q_ref[...]

    def side_a(i):
        k = L.block(i, 0)
        L.wait(g.at[k], i - 1)
        if i == 1:
            L.copy(lo(k), lo(k), 2, "a+")
        else:
            L.copy(hi(k), hi(k), 3, "a-")
        L.copy(g.at[k], g.at[k], 4 + 4 * i, "b+")
        L.copy(g.at[k], g.at[k], 5 + 4 * i, "b-")
        L.copy(g.at[k], g.at[k], 20 + 4 * i, "p")

    def far_a():
        k = L.block(3, 0)
        L.wait(lo(k), 2)
        L.wait(hi(k), 3)
        L.copy(g.at[k], g.at[k], 16, "b+")
        L.copy(g.at[k], g.at[k], 17, "b-")
        L.copy(g.at[k], g.at[k], 32, "p")

    def side_b(i):
        k = L.block(i, 1)
        L.wait(g.at[k], 4 + 4 * i)
        L.copy(lo(k), lo(k), 6 + 4 * i, "b+")
        L.copy(g.at[k], g.at[k], 21 + 4 * i, "p")
        k = L.block(i, 2)
        L.wait(g.at[k], 5 + 4 * i)
        L.copy(hi(k), hi(k), 7 + 4 * i, "b-")
        L.copy(g.at[k], g.at[k], 22 + 4 * i, "p")

    def far_b(i):
        k = L.block(i, 3)
        L.wait(lo(k), 6 + 4 * i)
        L.wait(hi(k), 7 + 4 * i)
        L.copy(g.at[k], g.at[k], 23 + 4 * i, "p")
        for j in range(4):
            k = L.partner_block(i, j)
            L.wait(g.at[k], 20 + 4 * i + j)

    def work(i):
        def block_of(n):
            other, j = n // 4, lax.rem(n, 4)
            core = L.core + other - 2 * L.core * other
            a = lax.rem(L.a * (1 - other) + L.b * other + OFF[i], 4)
            return index_of(core, a, j)

        def pick(n, carry):
            s = block_of(n)
            table = slot_tables(ids_ref[s] - first, pos_ref[s])
            info[s] = table
            one = jnp.concatenate([picks(table, c).astype(f32) for c in range(4)], axis=0)
            rows = jnp.dot(one.astype(jnp.bfloat16), g[s], preferred_element_type=f32)
            rec[s] = rows.astype(jnp.bfloat16).reshape(4, SLOTS, rows.shape[1])
            return carry

        lax.fori_loop(0, 8, pick, 0)

        def score(c, carry):
            rows = jnp.concatenate([rec[block_of(n), c] for n in range(8)], axis=0)
            out = lax.dot_general(rows, labels[c], (((1,), (1,)), ((), ())), preferred_element_type=f32)
            bias = jnp.sum(rows.astype(f32) * match[c].astype(f32), axis=1, keepdims=True)
            out = out + bias
            for n in range(8):
                scores[block_of(n), c] = out[n * SLOTS : (n + 1) * SLOTS]
            return carry

        lax.fori_loop(0, 4, score, 0)

        def stat(n, carry):
            s = block_of(n)
            table = info[s]
            leaf = lax.broadcasted_iota(jnp.int32, (SLOTS, LEAF), 1).astype(f32)
            parts = []
            for c in range(4):
                one = picks(table, c)
                val = scores[s, c]
                top = jnp.max(val, axis=1, keepdims=True)
                total = jnp.sum(jnp.exp(val - top), axis=1, keepdims=True)
                picked = jnp.sum(
                    jnp.where(leaf == target_column(table, one, c), val, 0.0), axis=1, keepdims=True
                )
                parts.append((one, top, total, picked))
            best = jnp.full((1, table.shape[1]), -BIG, f32)
            for one, top, total, picked in parts:
                best = jnp.maximum(best, jnp.max(jnp.where(one, top, -BIG), axis=0, keepdims=True))
            spread = jnp.zeros_like(best)
            chosen = jnp.zeros_like(best)
            for one, top, total, picked in parts:
                spread += jnp.sum(
                    jnp.where(one, total * jnp.exp(jnp.where(one, top - best, 0.0)), 0.0), axis=0, keepdims=True
                )
                chosen += jnp.sum(jnp.where(one, picked, 0.0), axis=0, keepdims=True)
            line = lax.broadcasted_iota(jnp.int32, (8, table.shape[1]), 0)
            st[s] = jnp.where(line == 0, best, jnp.where(line == 1, spread, chosen))
            return carry

        lax.fori_loop(0, 8, stat, 0)
        for core in range(2):
            for j in range(4):
                k = L.block(i, j) if core == 0 else L.partner_block(i, j)
                n = 8 * i + 4 * core + j
                pltpu.make_async_copy(scores.at[k], scores_out.at[k], out_sem.at[2 * n]).start()
                pltpu.make_async_copy(rec.at[k], rec_out.at[k], out_sem.at[2 * n + 1]).start()
                if n == 0:
                    continue
                pltpu.make_async_remote_copy(
                    src_ref=st.at[k], dst_ref=sr.at[L.me], send_sem=st_send.at[k], recv_sem=st_recv.at[L.me],
                    device_id={"label": k}, device_id_type=MESH,
                ).start()

    side_a(1)
    side_a(2)
    side_b(0)
    far_a()
    side_b(1)
    far_b(0)
    work(0)
    side_b(2)
    far_b(1)
    work(1)
    side_b(3)
    far_b(2)
    work(2)
    far_b(3)
    work(3)
    sr[own] = st[own]

    def stat_copy(k, arrive):
        return pltpu.make_async_remote_copy(
            src_ref=st.at[k], dst_ref=sr.at[k], send_sem=st_send.at[k], recv_sem=st_recv.at[k],
            device_id={"label": k}, device_id_type=MESH,
        )

    for k in peers:
        stat_copy(k, True).wait_recv()
    best = jnp.max(sr[:, 0:1, :], axis=0)
    lines = sr[...]
    spread = jnp.sum(lines[:, 1:2, :] * jnp.exp(lines[:, 0:1, :] - best[None]), axis=0)
    chosen = jnp.sum(lines[:, 2:3, :], axis=0)
    value = best + jnp.log(spread)
    losses[...] = jnp.broadcast_to(value - chosen, losses.shape)
    lse[own] = jnp.broadcast_to(value, lse.shape[1:])

    def lse_copy(dev, row):
        return pltpu.make_async_remote_copy(
            src_ref=lse.at[row], dst_ref=lse.at[row], send_sem=lse_send.at[dev], recv_sem=lse_recv.at[row],
            device_id={"label": dev}, device_id_type=MESH,
        )

    for k in peers:
        lse_copy(k, own).start()
    for k in peers:
        lse_copy(k, k).wait_recv()
    for k in peers:
        stat_copy(k, False).wait_send()
        lse_copy(k, own).wait_send()
    for i in range(4):
        for core in range(2):
            for j in range(4):
                k = L.block(i, j) if core == 0 else L.partner_block(i, j)
                n = 8 * i + 4 * core + j
                pltpu.make_async_copy(scores.at[k], scores_out.at[k], out_sem.at[2 * n]).wait()
                pltpu.make_async_copy(rec.at[k], rec_out.at[k], out_sem.at[2 * n + 1]).wait()
    L.drain()


def forward(q, labels, match, ids, pos):
    q_dev, width = q.shape
    vmem = pl.BlockSpec(memory_space=pltpu.VMEM)
    hbm = pl.BlockSpec(memory_space=pl.ANY)
    shape = jax.ShapeDtypeStruct
    f32, bf16, dma = jnp.float32, jnp.bfloat16, pltpu.SemaphoreType.DMA
    return pl.pallas_call(
        forward_kernel,
        out_shape=(
            shape((32, 4, SLOTS, LEAF), f32),
            shape((32, 4, SLOTS, width), bf16),
            shape((32, 8, q_dev), f32),
            shape((32, 8, q_dev), f32),
            shape((8, q_dev), f32),
        ),
        in_specs=[vmem] * 5,
        out_specs=(hbm, hbm, vmem, vmem, vmem),
        scratch_shapes=[
            pltpu.VMEM((32, q_dev, width), bf16),
            pltpu.VMEM((32, 4, SLOTS, LEAF), f32),
            pltpu.VMEM((32, 4, SLOTS, width), bf16),
            pltpu.VMEM((32, 8, q_dev), f32),
            pltpu.VMEM((32, 8, q_dev), f32),
            dma((36,)), dma((36,)), dma((32,)), dma((32,)), dma((32,)), dma((32,)), dma((64,)),
        ],
        compiler_params=pltpu.CompilerParams(
            collective_id=0, has_side_effects=True, vmem_limit_bytes=60 * 1024 * 1024
        ),
    )(q, labels, match, ids, pos)


def backward_kernel(scores, rec, info, lse, labels, match, partial, label_part, local_sum,
                    delta, coef, grads, held):
    f32, bf16 = jnp.float32, jnp.bfloat16
    step = pl.program_id(0)
    blocks = scores.shape[0]

    @pl.when(step == 0)
    def _():
        local_sum[...] = jnp.zeros_like(local_sum)

    def part(n, carry):
        table = info[n]
        leaf = lax.broadcasted_iota(jnp.int32, (SLOTS, LEAF), 1).astype(f32)
        log_sum = lse[n, 0:1]
        for c in range(4):
            one = picks(table, c)
            used = jnp.sum(jnp.where(one, 1.0, 0.0), axis=1, keepdims=True) > 0.5
            norm = jnp.sum(jnp.where(one, log_sum, 0.0), axis=1, keepdims=True)
            norm = jnp.where(used, norm, BIG)
            hit = leaf == target_column(table, one, c)
            value = jnp.exp(scores[n, c] - norm) - hit.astype(f32)
            total = jnp.sum(value, axis=1, keepdims=True).astype(bf16)
            rows = pl.ds(pl.multiple_of((step * blocks + n) * SLOTS, 16), SLOTS)
            delta[c, rows] = value.astype(bf16)
            coef[c, pl.ds(pl.multiple_of(n * SLOTS, 16), SLOTS)] = jnp.broadcast_to(total.astype(f32), (SLOTS, 128))
            local_sum[c] += jnp.sum(total.astype(f32) * rec[n, c].astype(f32), axis=0, keepdims=True)
        return carry

    lax.fori_loop(0, blocks, part, 0)

    def slot(c, carry):
        rows = pl.ds(pl.multiple_of(step * blocks * SLOTS, 16), blocks * SLOTS)
        out = jnp.dot(delta[c, rows], labels[c], preferred_element_type=f32)
        out = out + coef[c][:, 0:1] * match[c].astype(f32)
        out = out.astype(bf16)
        for n in range(blocks):
            grads[n, pl.ds(pl.multiple_of(c * SLOTS, 16), SLOTS)] = out[n * SLOTS : (n + 1) * SLOTS]
        return carry

    lax.fori_loop(0, 4, slot, 0)

    def back(n, carry):
        table = info[n]
        one = jnp.concatenate([picks(table, c).astype(f32) for c in range(4)], axis=0).astype(bf16)
        out = lax.dot_general(one, grads[n], (((0,), (0,)), ((), ())), preferred_element_type=f32)
        partial[n] = out.astype(bf16)
        return carry

    lax.fori_loop(0, blocks, back, 0)

    for n in range(blocks):
        held[:, pl.ds(pl.multiple_of((step * blocks + n) * SLOTS, 16), SLOTS)] = rec[n]

    @pl.when(step == pl.num_programs(0) - 1)
    def _():
        def gather_part(c, carry):
            out = lax.dot_general(delta[c], held[c], (((0,), (0,)), ((), ())), preferred_element_type=f32)
            label_part[c] = out.astype(bf16)
            return carry

        lax.fori_loop(0, 4, gather_part, 0)


def backward(scores, rec, info, lse, labels, match):
    n, _, _, width = rec.shape
    q_dev = info.shape[2]
    f32, bf16 = jnp.float32, jnp.bfloat16
    group = 8
    vmem = pl.BlockSpec(memory_space=pltpu.VMEM)
    shape = jax.ShapeDtypeStruct
    return pl.pallas_call(
        backward_kernel,
        grid=(n // group,),
        out_shape=(
            shape((n, q_dev, width), bf16),
            shape((4, LEAF, width), bf16),
            shape((4, 1, width), f32),
        ),
        in_specs=[
            pl.BlockSpec((group, 4, SLOTS, LEAF), lambda i: (i, 0, 0, 0)),
            pl.BlockSpec((group, 4, SLOTS, width), lambda i: (i, 0, 0, 0)),
            pl.BlockSpec((group, 8, q_dev), lambda i: (i, 0, 0)),
            pl.BlockSpec((group, 8, q_dev), lambda i: (i, 0, 0)),
            vmem,
            vmem,
        ],
        out_specs=(
            pl.BlockSpec((group, q_dev, width), lambda i: (i, 0, 0)),
            vmem,
            vmem,
        ),
        scratch_shapes=[
            pltpu.VMEM((4, n * SLOTS, LEAF), bf16),
            pltpu.VMEM((4, group * SLOTS, 128), f32),
            pltpu.VMEM((group, 4 * SLOTS, width), bf16),
            pltpu.VMEM((4, n * SLOTS, width), bf16),
        ],
        compiler_params=pltpu.CompilerParams(vmem_limit_bytes=60 * 1024 * 1024),
    )(scores, rec, info, lse, labels, match)


def scatter_kernel(p, out, t, u, pr, bh, bf, ah, af, send, recv):
    L = Links(send, recv)
    L.meet()
    half = p.shape[1] // 2
    f32 = jnp.float32
    ORDER = [(i, 3) for i in (3, 1, 2, 0)] + [(i, j) for i in (3, 1, 2, 0) for j in (1, 2)] + [(i, 0) for i in (3, 1, 2, 0)]
    for i, j in ORDER:
        L.copy(p.at[L.partner_block(i, j)], pr.at[4 * i + j], 4 * i + j, "p")
    LO, HI = pl.ds(0, half), pl.ds(half, half)
    def both(i, j):
        L.wait(pr.at[4 * i + j], 4 * i + j)
        return lambda s: p[L.block(i, j), s].astype(f32) + pr[4 * i + j, s].astype(f32)
    for i in (3, 1, 2, 0):
        s = both(i, 3)
        n = 3 * i + 2
        t[n] = s(slice(None)).astype(t.dtype)
        L.copy(t.at[n, LO], bh.at[i, 0], 16 + 4 * i, "b+")
        L.copy(t.at[n, HI], bh.at[i, 1], 17 + 4 * i, "b-")
    for i in (3, 1, 2, 0):
        s = both(i, 2)
        n = 3 * i + 1
        L.wait(bh.at[i, 0], 16 + 4 * i)
        t[n, LO] = (s(LO) + bh[i, 0].astype(f32)).astype(t.dtype)
        t[n, HI] = s(HI).astype(t.dtype)
        L.copy(t.at[n], bf.at[i, 0], 18 + 4 * i, "b+")
        s = both(i, 1)
        n = 3 * i
        L.wait(bh.at[i, 1], 17 + 4 * i)
        t[n, HI] = (s(HI) + bh[i, 1].astype(f32)).astype(t.dtype)
        t[n, LO] = s(LO).astype(t.dtype)
        L.copy(t.at[n], bf.at[i, 1], 19 + 4 * i, "b-")
    def column(i):
        s = both(i, 0)
        L.wait(bf.at[i, 0], 18 + 4 * i)
        L.wait(bf.at[i, 1], 19 + 4 * i)
        return lambda r: s(r) + bf[i, 0, r].astype(f32) + bf[i, 1, r].astype(f32)
    s = column(3)
    u[2] = s(slice(None)).astype(u.dtype)
    L.copy(u.at[2, LO], ah.at[0], 32, "a+")
    L.copy(u.at[2, HI], ah.at[1], 33, "a-")
    s = column(1)
    L.wait(ah.at[1], 33)
    u[0, HI] = (s(HI) + ah[1].astype(f32)).astype(u.dtype)
    u[0, LO] = s(LO).astype(u.dtype)
    L.copy(u.at[0], af.at[1], 35, "a-")
    s = column(2)
    L.wait(ah.at[0], 32)
    u[1, LO] = (s(LO) + ah[0].astype(f32)).astype(u.dtype)
    u[1, HI] = s(HI).astype(u.dtype)
    L.copy(u.at[1], af.at[0], 34, "a+")
    s = column(0)
    L.wait(af.at[0], 34)
    L.wait(af.at[1], 35)
    out[...] = s(slice(None)) + af[0].astype(f32) + af[1].astype(f32)
    L.drain()

def scatter(p):
    n, r, w = p.shape
    bf16 = jnp.bfloat16
    return pl.pallas_call(
        scatter_kernel,
        out_shape=jax.ShapeDtypeStruct((r, w), jnp.float32),
        in_specs=[pl.BlockSpec(memory_space=pltpu.VMEM)],
        out_specs=pl.BlockSpec(memory_space=pltpu.VMEM),
        scratch_shapes=[pltpu.VMEM((12, r, w), bf16), pltpu.VMEM((3, r, w), bf16), pltpu.VMEM((16, r, w), bf16),
            pltpu.VMEM((4, 2, r // 2, w), bf16), pltpu.VMEM((4, 2, r, w), bf16), pltpu.VMEM((2, r // 2, w), bf16), pltpu.VMEM((2, r, w), bf16),
            pltpu.SemaphoreType.DMA((36,)), pltpu.SemaphoreType.DMA((36,))],
        compiler_params=pltpu.CompilerParams(collective_id=1, has_side_effects=True),
    )(p)


def over_copies(shard, axis):
    devices = lax.axis_size(axis)
    spread = jnp.broadcast_to(shard[None], (devices, *shard.shape))
    return lax.all_to_all(spread, axis, 0, 0, tiled=True).sum(axis=0)


def body(queries, labels, matcher, cluster_ids, positives):
    q_dev, width = queries.shape
    cl_dev = labels.shape[0]
    n_label = lax.axis_size("label")
    first = lax.axis_index("label") * cl_dev
    match = lax.dynamic_slice_in_dim(matcher, first, cl_dev, 0).reshape(cl_dev, 1, width)
    ids = cluster_ids.reshape(n_label, q_dev, K).transpose(0, 2, 1)
    pos = positives.reshape(n_label, 1, q_dev)
    scores, received, info, lse, losses = forward(queries, labels, match, ids, pos)
    partial, label_part, local_sum = backward(scores, received, info, lse, labels, match)
    label_grads = lax.psum_scatter(
        label_part, "dp", scatter_dimension=1, tiled=True
    ).astype(jnp.float32)
    query_grads = scatter(partial)
    local_sum = over_copies(local_sum.reshape(cl_dev, width), "dp")
    matcher_grads = lax.all_gather(local_sum, "label", axis=0, tiled=True)
    return (losses[0], query_grads, label_grads, matcher_grads)


def solution(mesh):
    return jax.shard_map(
        body,
        mesh=mesh,
        in_specs=(P(("dp", "label"), None), P("label", None, None), P(), P("dp", None), P("dp")),
        out_specs=(P(("dp", "label")), P(("dp", "label"), None), P("label", "dp", None), P()),
        check_vma=False,
    )
```

```python
import jax
import jax.numpy as jnp
from jax import lax
from jax.experimental import pallas as pl
from jax.experimental.pallas import tpu as pltpu
from jax.sharding import PartitionSpec as P

LEAF = 512
K = 16
BIG = 1e30

MESH = pl.DeviceIdType.MESH

def place():
    me = lax.axis_index("label")
    core = lax.rem(me, 2)
    x = lax.rem(me // 2, 4)
    y = me // 8
    a = x * (1 - core) + y * core
    b = y * (1 - core) + x * core
    return me, core, a, b

def index_of(core, a, b):
    x = a * (1 - core) + b * core
    y = b * (1 - core) + a * core
    return (y * 4 + x) * 2 + core

OFF = (0, 3, 1, 2)

class Links:
    def __init__(self, send, recv):
        self.me, self.core, self.a, self.b = place()
        self.send, self.recv, self.sent = send, recv, []
        c, a, b = self.core, self.a, self.b
        self.partner = self.me + 1 - 2 * c
        self.dev = {
            "a-": index_of(c, lax.rem(a + 3, 4), b),
            "a+": index_of(c, lax.rem(a + 1, 4), b),
            "b-": index_of(c, a, lax.rem(b + 3, 4)),
            "b+": index_of(c, a, lax.rem(b + 1, 4)),
            "p": self.partner,
        }
    def block(self, i, j):
        return index_of(self.core, lax.rem(self.a + OFF[i], 4), lax.rem(self.b + OFF[j], 4))
    def partner_block(self, i, j):
        return index_of(1 - self.core, lax.rem(self.b + OFF[i], 4), lax.rem(self.a + OFF[j], 4))
    def meet(self, peers=None):
        barrier = pltpu.get_barrier_semaphore()
        peers = list(self.dev.values()) if peers is None else peers
        for d in peers:
            pl.semaphore_signal(barrier, inc=1, device_id={"label": d}, device_id_type=MESH)
        pl.semaphore_wait(barrier, len(peers))
    def copy(self, src, dst, slot, to):
        n = len(self.sent)
        c = pltpu.make_async_remote_copy(src_ref=src, dst_ref=dst, send_sem=self.send.at[n],
            recv_sem=self.recv.at[slot], device_id={"label": self.dev[to]}, device_id_type=MESH)
        c.start()
        self.sent.append(c)
    def wait(self, dst, slot):
        pltpu.make_async_remote_copy(src_ref=dst, dst_ref=dst, send_sem=self.send.at[0],
            recv_sem=self.recv.at[slot], device_id={"label": self.partner}, device_id_type=MESH).wait_recv()
    def drain(self):
        for c in self.sent:
            c.wait_send()


SLOTS = 48


def slot_tables(ids, pos):
    f32 = jnp.float32
    n = ids.shape[1]
    rows = lax.broadcasted_iota(jnp.int32, ids.shape, 0)
    pos_cluster = jnp.sum(
        jnp.where(rows == (pos >> 9), ids, 0).astype(f32), axis=0, keepdims=True
    )
    line = lax.broadcasted_iota(jnp.int32, (8, n), 0)
    named = jnp.zeros((8, n), f32)
    for c in range(4):
        hit = jnp.sum((ids == c).astype(f32), axis=0, keepdims=True)
        named = jnp.where(line == c, hit, named)
    earlier = (
        lax.broadcasted_iota(jnp.int32, (n, n), 0) < lax.broadcasted_iota(jnp.int32, (n, n), 1)
    ).astype(f32)
    rank = jnp.dot(
        named.astype(jnp.bfloat16), earlier.astype(jnp.bfloat16), preferred_element_type=f32
    )
    code = jnp.where(named > 0.5, rank, -1.0)
    target = ((pos & (LEAF - 1)) + 1).astype(f32)
    targets = jnp.where(pos_cluster == (line - 4).astype(f32), target, 0.0)
    return jnp.where(line < 4, code, targets)


def picks(info, c):
    r = lax.broadcasted_iota(jnp.int32, (SLOTS, info.shape[1]), 0).astype(jnp.float32)
    return info[c : c + 1] == r


def target_column(info, pick, c):
    return jnp.sum(jnp.where(pick, info[4 + c : 5 + c], 0.0), axis=1, keepdims=True) - 1.0


def forward_kernel(q_ref, labels, match, ids_ref, pos_ref, scores_out, rec_out, info, lse, losses,
                   g, scores, rec, st, sr, send, recv, st_send, st_recv, lse_send, lse_recv, out_sem):
    f32 = jnp.float32
    L = Links(send, recv)
    peers = [(k, L.block(i, j)) for k, (i, j) in enumerate([(i, j) for i in range(4) for j in range(4)])]
    peers = [d for k, d in peers if k > 0]
    peers += [L.partner_block(i, j) for i in range(4) for j in range(4)]
    L.meet(peers)
    half = q_ref.shape[0] // 2
    first = L.me * 4
    lo = lambda k: g.at[k, pl.ds(0, half)]
    hi = lambda k: g.at[k, pl.ds(half, half)]
    own = L.block(0, 0)
    for to, slot in (("a+", 0), ("a-", 1), ("b+", 4), ("b-", 5), ("p", 20)):
        L.copy(q_ref, g.at[own], slot, to)
    g[own] = q_ref[...]

    def side_a(i):
        k = L.block(i, 0)
        L.wait(g.at[k], i - 1)
        if i == 1:
            L.copy(lo(k), lo(k), 2, "a+")
        else:
            L.copy(hi(k), hi(k), 3, "a-")
        L.copy(g.at[k], g.at[k], 4 + 4 * i, "b+")
        L.copy(g.at[k], g.at[k], 5 + 4 * i, "b-")
        L.copy(g.at[k], g.at[k], 20 + 4 * i, "p")

    def far_a():
        k = L.block(3, 0)
        L.wait(lo(k), 2)
        L.wait(hi(k), 3)
        L.copy(g.at[k], g.at[k], 16, "b+")
        L.copy(g.at[k], g.at[k], 17, "b-")
        L.copy(g.at[k], g.at[k], 32, "p")

    def side_b(i):
        k = L.block(i, 1)
        L.wait(g.at[k], 4 + 4 * i)
        L.copy(lo(k), lo(k), 6 + 4 * i, "b+")
        L.copy(g.at[k], g.at[k], 21 + 4 * i, "p")
        k = L.block(i, 2)
        L.wait(g.at[k], 5 + 4 * i)
        L.copy(hi(k), hi(k), 7 + 4 * i, "b-")
        L.copy(g.at[k], g.at[k], 22 + 4 * i, "p")

    def far_b(i):
        k = L.block(i, 3)
        L.wait(lo(k), 6 + 4 * i)
        L.wait(hi(k), 7 + 4 * i)
        L.copy(g.at[k], g.at[k], 23 + 4 * i, "p")
        for j in range(4):
            k = L.partner_block(i, j)
            L.wait(g.at[k], 20 + 4 * i + j)

    def work(i):
        def block_of(n):
            other, j = n // 4, lax.rem(n, 4)
            core = L.core + other - 2 * L.core * other
            a = lax.rem(L.a * (1 - other) + L.b * other + OFF[i], 4)
            return index_of(core, a, j)

        def pick(n, carry):
            s = block_of(n)
            table = slot_tables(ids_ref[s] - first, pos_ref[s])
            info[s] = table
            one = jnp.concatenate([picks(table, c).astype(f32) for c in range(4)], axis=0)
            rows = jnp.dot(one.astype(jnp.bfloat16), g[s], preferred_element_type=f32)
            rec[s] = rows.astype(jnp.bfloat16).reshape(4, SLOTS, rows.shape[1])
            return carry

        lax.fori_loop(0, 8, pick, 0)

        def score(c, carry):
            rows = jnp.concatenate([rec[block_of(n), c] for n in range(8)], axis=0)
            out = lax.dot_general(rows, labels[c], (((1,), (1,)), ((), ())), preferred_element_type=f32)
            bias = jnp.sum(rows.astype(f32) * match[c].astype(f32), axis=1, keepdims=True)
            out = out + bias
            for n in range(8):
                scores[block_of(n), c] = out[n * SLOTS : (n + 1) * SLOTS]
            return carry

        lax.fori_loop(0, 4, score, 0)

        def stat(n, carry):
            s = block_of(n)
            table = info[s]
            leaf = lax.broadcasted_iota(jnp.int32, (SLOTS, LEAF), 1).astype(f32)
            parts = []
            for c in range(4):
                one = picks(table, c)
                val = scores[s, c]
                top = jnp.max(val, axis=1, keepdims=True)
                total = jnp.sum(jnp.exp(val - top), axis=1, keepdims=True)
                picked = jnp.sum(
                    jnp.where(leaf == target_column(table, one, c), val, 0.0), axis=1, keepdims=True
                )
                parts.append((one, top, total, picked))
            best = jnp.full((1, table.shape[1]), -BIG, f32)
            for one, top, total, picked in parts:
                best = jnp.maximum(best, jnp.max(jnp.where(one, top, -BIG), axis=0, keepdims=True))
            spread = jnp.zeros_like(best)
            chosen = jnp.zeros_like(best)
            for one, top, total, picked in parts:
                spread += jnp.sum(
                    jnp.where(one, total * jnp.exp(jnp.where(one, top - best, 0.0)), 0.0), axis=0, keepdims=True
                )
                chosen += jnp.sum(jnp.where(one, picked, 0.0), axis=0, keepdims=True)
            line = lax.broadcasted_iota(jnp.int32, (8, table.shape[1]), 0)
            st[s] = jnp.where(line == 0, best, jnp.where(line == 1, spread, chosen))
            return carry

        lax.fori_loop(0, 8, stat, 0)
        for core in range(2):
            for j in range(4):
                k = L.block(i, j) if core == 0 else L.partner_block(i, j)
                n = 8 * i + 4 * core + j
                pltpu.make_async_copy(scores.at[k], scores_out.at[k], out_sem.at[2 * n]).start()
                pltpu.make_async_copy(rec.at[k], rec_out.at[k], out_sem.at[2 * n + 1]).start()
                if n == 0:
                    continue
                pltpu.make_async_remote_copy(
                    src_ref=st.at[k], dst_ref=sr.at[L.me], send_sem=st_send.at[k], recv_sem=st_recv.at[L.me],
                    device_id={"label": k}, device_id_type=MESH,
                ).start()

    side_a(1)
    side_a(2)
    side_b(0)
    far_a()
    side_b(1)
    far_b(0)
    work(0)
    side_b(2)
    far_b(1)
    work(1)
    side_b(3)
    far_b(2)
    work(2)
    far_b(3)
    work(3)
    sr[own] = st[own]

    def stat_copy(k, arrive):
        return pltpu.make_async_remote_copy(
            src_ref=st.at[k], dst_ref=sr.at[k], send_sem=st_send.at[k], recv_sem=st_recv.at[k],
            device_id={"label": k}, device_id_type=MESH,
        )

    for k in peers:
        stat_copy(k, True).wait_recv()
    best = jnp.max(sr[:, 0:1, :], axis=0)
    lines = sr[...]
    spread = jnp.sum(lines[:, 1:2, :] * jnp.exp(lines[:, 0:1, :] - best[None]), axis=0)
    chosen = jnp.sum(lines[:, 2:3, :], axis=0)
    value = best + jnp.log(spread)
    losses[...] = jnp.broadcast_to(value - chosen, losses.shape)
    lse[own] = jnp.broadcast_to(value, lse.shape[1:])

    def lse_copy(dev, row):
        return pltpu.make_async_remote_copy(
            src_ref=lse.at[row], dst_ref=lse.at[row], send_sem=lse_send.at[dev], recv_sem=lse_recv.at[row],
            device_id={"label": dev}, device_id_type=MESH,
        )

    for k in peers:
        lse_copy(k, own).start()
    for k in peers:
        lse_copy(k, k).wait_recv()
    for k in peers:
        stat_copy(k, False).wait_send()
        lse_copy(k, own).wait_send()
    for i in range(4):
        for core in range(2):
            for j in range(4):
                k = L.block(i, j) if core == 0 else L.partner_block(i, j)
                n = 8 * i + 4 * core + j
                pltpu.make_async_copy(scores.at[k], scores_out.at[k], out_sem.at[2 * n]).wait()
                pltpu.make_async_copy(rec.at[k], rec_out.at[k], out_sem.at[2 * n + 1]).wait()
    L.drain()


def forward(q, labels, match, ids, pos):
    q_dev, width = q.shape
    vmem = pl.BlockSpec(memory_space=pltpu.VMEM)
    hbm = pl.BlockSpec(memory_space=pl.ANY)
    shape = jax.ShapeDtypeStruct
    f32, bf16, dma = jnp.float32, jnp.bfloat16, pltpu.SemaphoreType.DMA
    return pl.pallas_call(
        forward_kernel,
        out_shape=(
            shape((32, 4, SLOTS, LEAF), f32),
            shape((32, 4, SLOTS, width), bf16),
            shape((32, 8, q_dev), f32),
            shape((32, 8, q_dev), f32),
            shape((8, q_dev), f32),
        ),
        in_specs=[vmem] * 5,
        out_specs=(hbm, hbm, vmem, vmem, vmem),
        scratch_shapes=[
            pltpu.VMEM((32, q_dev, width), bf16),
            pltpu.VMEM((32, 4, SLOTS, LEAF), f32),
            pltpu.VMEM((32, 4, SLOTS, width), bf16),
            pltpu.VMEM((32, 8, q_dev), f32),
            pltpu.VMEM((32, 8, q_dev), f32),
            dma((36,)), dma((36,)), dma((32,)), dma((32,)), dma((32,)), dma((32,)), dma((64,)),
        ],
        compiler_params=pltpu.CompilerParams(
            collective_id=0, has_side_effects=True, vmem_limit_bytes=60 * 1024 * 1024
        ),
    )(q, labels, match, ids, pos)


def backward_kernel(scores, rec, info, lse, labels, match, partial, label_part, local_sum,
                    delta, coef, grads, held):
    f32, bf16 = jnp.float32, jnp.bfloat16
    step = pl.program_id(0)
    blocks = scores.shape[0]

    @pl.when(step == 0)
    def _():
        local_sum[...] = jnp.zeros_like(local_sum)

    def part(n, carry):
        table = info[n]
        leaf = lax.broadcasted_iota(jnp.int32, (SLOTS, LEAF), 1).astype(f32)
        log_sum = lse[n, 0:1]
        for c in range(4):
            one = picks(table, c)
            used = jnp.sum(jnp.where(one, 1.0, 0.0), axis=1, keepdims=True) > 0.5
            norm = jnp.sum(jnp.where(one, log_sum, 0.0), axis=1, keepdims=True)
            norm = jnp.where(used, norm, BIG)
            hit = leaf == target_column(table, one, c)
            value = jnp.exp(scores[n, c] - norm) - hit.astype(f32)
            total = jnp.sum(value, axis=1, keepdims=True).astype(bf16)
            rows = pl.ds(pl.multiple_of((step * blocks + n) * SLOTS, 16), SLOTS)
            delta[c, rows] = value.astype(bf16)
            coef[c, pl.ds(pl.multiple_of(n * SLOTS, 16), SLOTS)] = jnp.broadcast_to(total.astype(f32), (SLOTS, 128))
            local_sum[c] += jnp.sum(total.astype(f32) * rec[n, c].astype(f32), axis=0, keepdims=True)
        return carry

    lax.fori_loop(0, blocks, part, 0)

    def slot(c, carry):
        rows = pl.ds(pl.multiple_of(step * blocks * SLOTS, 16), blocks * SLOTS)
        out = jnp.dot(delta[c, rows], labels[c], preferred_element_type=f32)
        out = out + coef[c][:, 0:1] * match[c].astype(f32)
        out = out.astype(bf16)
        for n in range(blocks):
            grads[n, pl.ds(pl.multiple_of(c * SLOTS, 16), SLOTS)] = out[n * SLOTS : (n + 1) * SLOTS]
        return carry

    lax.fori_loop(0, 4, slot, 0)

    def back(n, carry):
        table = info[n]
        one = jnp.concatenate([picks(table, c).astype(f32) for c in range(4)], axis=0).astype(bf16)
        out = lax.dot_general(one, grads[n], (((0,), (0,)), ((), ())), preferred_element_type=f32)
        partial[n] = out.astype(bf16)
        return carry

    lax.fori_loop(0, blocks, back, 0)

    for n in range(blocks):
        held[:, pl.ds(pl.multiple_of((step * blocks + n) * SLOTS, 16), SLOTS)] = rec[n]

    @pl.when(step == pl.num_programs(0) - 1)
    def _():
        def gather_part(c, carry):
            out = lax.dot_general(delta[c], held[c], (((0,), (0,)), ((), ())), preferred_element_type=f32)
            label_part[c] = out.astype(bf16)
            return carry

        lax.fori_loop(0, 4, gather_part, 0)


def backward(scores, rec, info, lse, labels, match):
    n, _, _, width = rec.shape
    q_dev = info.shape[2]
    f32, bf16 = jnp.float32, jnp.bfloat16
    group = 8
    vmem = pl.BlockSpec(memory_space=pltpu.VMEM)
    shape = jax.ShapeDtypeStruct
    return pl.pallas_call(
        backward_kernel,
        grid=(n // group,),
        out_shape=(
            shape((n, q_dev, width), bf16),
            shape((4, LEAF, width), bf16),
            shape((4, 1, width), f32),
        ),
        in_specs=[
            pl.BlockSpec((group, 4, SLOTS, LEAF), lambda i: (i, 0, 0, 0)),
            pl.BlockSpec((group, 4, SLOTS, width), lambda i: (i, 0, 0, 0)),
            pl.BlockSpec((group, 8, q_dev), lambda i: (i, 0, 0)),
            pl.BlockSpec((group, 8, q_dev), lambda i: (i, 0, 0)),
            vmem,
            vmem,
        ],
        out_specs=(
            pl.BlockSpec((group, q_dev, width), lambda i: (i, 0, 0)),
            vmem,
            vmem,
        ),
        scratch_shapes=[
            pltpu.VMEM((4, n * SLOTS, LEAF), bf16),
            pltpu.VMEM((4, group * SLOTS, 128), f32),
            pltpu.VMEM((group, 4 * SLOTS, width), bf16),
            pltpu.VMEM((4, n * SLOTS, width), bf16),
        ],
        compiler_params=pltpu.CompilerParams(vmem_limit_bytes=60 * 1024 * 1024),
    )(scores, rec, info, lse, labels, match)


class Column:
    def __init__(self, links):
        self.z = lax.axis_index("dp")
        self.links = links

    def copy(self, src, dst, slot, off):
        L = self.links
        n = len(L.sent)
        c = pltpu.make_async_remote_copy(
            src_ref=src, dst_ref=dst, send_sem=L.send.at[n], recv_sem=L.recv.at[slot],
            device_id={"dp": lax.rem(self.z + off, 4)}, device_id_type=MESH,
        )
        c.start()
        L.sent.append(c)


def scatter_kernel(p, lp, ls, out, label_out, mout, t_all, u, pr, bh, bf, ah, af, zt, zh, zf, mz, send, recv, m_recv):
    L = Links(send, recv)
    Z = Column(L)
    z = Z.z
    peers = [L.block(i, j) for i in range(4) for j in range(4)][1:]
    peers += [L.partner_block(i, j) for i in range(4) for j in range(4)]
    barrier = pltpu.get_barrier_semaphore()
    for d in peers:
        pl.semaphore_signal(barrier, inc=1, device_id={"label": d}, device_id_type=MESH)
    for off in (1, 2, 3):
        pl.semaphore_signal(barrier, inc=1, device_id={"dp": lax.rem(z + off, 4)}, device_id_type=MESH)
    pl.semaphore_wait(barrier, 34)
    half = p.shape[1] // 2
    f32 = jnp.float32
    rows_z = label_out.shape[1]

    def rows(off):
        return pl.ds(pl.multiple_of(lax.rem(z + off, 4) * rows_z, rows_z), rows_z)

    PAIRS = pl.ds(0, 2), pl.ds(2, 2)
    for off in (1, 2, 3):
        Z.copy(ls.at[lax.rem(z + off, 4)], mz.at[z], 41 + off, off)
    ORDER = [(i, 3) for i in (3, 1, 2, 0)] + [(i, j) for i in (3, 1, 2, 0) for j in (1, 2)] + [(i, 0) for i in (3, 1, 2, 0)]
    for i, j in ORDER:
        L.copy(p.at[L.partner_block(i, j)], pr.at[4 * i + j], 4 * i + j, "p")
    Z.copy(lp.at[PAIRS[0], rows(2)], zh.at[0], 36, 1)
    Z.copy(lp.at[PAIRS[1], rows(2)], zh.at[1], 37, 3)
    LO, HI = pl.ds(0, half), pl.ds(half, half)
    mz[z] = ls[z]

    def both(i, j):
        L.wait(pr.at[4 * i + j], 4 * i + j)
        return lambda s: p[L.block(i, j), s].astype(f32) + pr[4 * i + j, s].astype(f32)

    for i in (3, 1, 2, 0):
        s = both(i, 3)
        t = t_all.at[3 * i + 2]
        t[...] = s(slice(None)).astype(t.dtype)
        L.copy(t.at[LO], bh.at[i, 0], 16 + 4 * i, "b+")
        L.copy(t.at[HI], bh.at[i, 1], 17 + 4 * i, "b-")
    for off in (1, 2, 3):
        L.wait(mz.at[lax.rem(z + 4 - off, 4)], 41 + off)
    mout[z, L.me] = mz[0] + mz[1] + mz[2] + mz[3]

    def row_copy(dev, row):
        return pltpu.make_async_remote_copy(
            src_ref=mout.at[z, row], dst_ref=mout.at[z, row], send_sem=m_recv.at[1, dev], recv_sem=m_recv.at[0, row],
            device_id={"label": dev}, device_id_type=MESH,
        )

    for k in peers:
        row_copy(k, L.me).start()
    L.wait(zh.at[0], 36)
    zt[1, 0:2] = (lp[PAIRS[0], rows(1)].astype(f32) + zh[0].astype(f32)).astype(zt.dtype)
    zt[1, 2:4] = lp[PAIRS[1], rows(1)]
    Z.copy(zt.at[1], zf.at[0], 38, 1)
    L.wait(zh.at[1], 37)
    zt[0, 2:4] = (lp[PAIRS[1], rows(3)].astype(f32) + zh[1].astype(f32)).astype(zt.dtype)
    zt[0, 0:2] = lp[PAIRS[0], rows(3)]
    Z.copy(zt.at[0], zf.at[1], 39, 3)
    for i in (3, 1, 2, 0):
        s = both(i, 2)
        t = t_all.at[3 * i + 1]
        L.wait(bh.at[i, 0], 16 + 4 * i)
        t[LO] = (s(LO) + bh[i, 0].astype(f32)).astype(t.dtype)
        t[HI] = s(HI).astype(t.dtype)
        L.copy(t, bf.at[i, 0], 18 + 4 * i, "b+")
        s = both(i, 1)
        t = t_all.at[3 * i + 0]
        L.wait(bh.at[i, 1], 17 + 4 * i)
        t[HI] = (s(HI) + bh[i, 1].astype(f32)).astype(t.dtype)
        t[LO] = s(LO).astype(t.dtype)
        L.copy(t, bf.at[i, 1], 19 + 4 * i, "b-")
    for k in peers:
        row_copy(k, k).wait_recv()
    for off in (1, 2, 3):
        Z.copy(mout.at[z], mout.at[z], 44 + off, off)

    def column(i):
        s = both(i, 0)
        L.wait(bf.at[i, 0], 18 + 4 * i)
        L.wait(bf.at[i, 1], 19 + 4 * i)
        return lambda r: s(r) + bf[i, 0, r].astype(f32) + bf[i, 1, r].astype(f32)

    s = column(3)
    u[2] = s(slice(None)).astype(u.dtype)
    L.copy(u.at[2, LO], ah.at[0], 32, "a+")
    L.copy(u.at[2, HI], ah.at[1], 33, "a-")
    s = column(1)
    L.wait(ah.at[1], 33)
    u[0, HI] = (s(HI) + ah[1].astype(f32)).astype(u.dtype)
    u[0, LO] = s(LO).astype(u.dtype)
    L.copy(u.at[0], af.at[1], 35, "a-")
    s = column(2)
    L.wait(ah.at[0], 32)
    u[1, LO] = (s(LO) + ah[0].astype(f32)).astype(u.dtype)
    u[1, HI] = s(HI).astype(u.dtype)
    L.copy(u.at[1], af.at[0], 34, "a+")
    L.wait(zf.at[0], 38)
    L.wait(zf.at[1], 39)
    label_out[...] = lp[:, rows(0)].astype(f32) + zf[0].astype(f32) + zf[1].astype(f32)
    s = column(0)
    L.wait(af.at[0], 34)
    L.wait(af.at[1], 35)
    out[...] = s(slice(None)) + af[0].astype(f32) + af[1].astype(f32)
    for off in (1, 2, 3):
        L.wait(mout.at[lax.rem(z + 4 - off, 4)], 44 + off)
    for k in peers:
        row_copy(k, L.me).wait_send()
    L.drain()


def scatter(p, lp, ls):
    n, r, w = p.shape
    clusters, leaf, _ = lp.shape
    f32, bf16, dma = jnp.float32, jnp.bfloat16, pltpu.SemaphoreType.DMA
    vmem = pl.BlockSpec(memory_space=pltpu.VMEM)
    shape = jax.ShapeDtypeStruct
    return pl.pallas_call(
        scatter_kernel,
        out_shape=(shape((r, w), f32), shape((clusters, leaf // 4, w), f32), shape((4, n, 1, w), f32)),
        in_specs=[vmem] * 3,
        out_specs=(vmem,) * 3,
        scratch_shapes=[
            pltpu.VMEM((12, r, w), bf16),
            pltpu.VMEM((3, r, w), bf16),
            pltpu.VMEM((16, r, w), bf16),
            pltpu.VMEM((4, 2, r // 2, w), bf16),
            pltpu.VMEM((4, 2, r, w), bf16),
            pltpu.VMEM((2, r // 2, w), bf16),
            pltpu.VMEM((2, r, w), bf16),
            pltpu.VMEM((2, clusters, leaf // 4, w), bf16),
            pltpu.VMEM((2, 2, leaf // 4, w), bf16),
            pltpu.VMEM((2, clusters, leaf // 4, w), bf16),
            pltpu.VMEM((4, 1, w), f32),
            dma((52,)),
            dma((48,)),
            dma((2, 32)),
        ],
        compiler_params=pltpu.CompilerParams(
            collective_id=1, has_side_effects=True, vmem_limit_bytes=60 * 1024 * 1024
        ),
    )(p, lp, ls)


def body(queries, labels, matcher, cluster_ids, positives):
    q_dev, width = queries.shape
    cl_dev = labels.shape[0]
    n_label = lax.axis_size("label")
    first = lax.axis_index("label") * cl_dev
    match = lax.dynamic_slice_in_dim(matcher, first, cl_dev, 0).reshape(cl_dev, 1, width)
    ids = cluster_ids.reshape(n_label, q_dev, K).transpose(0, 2, 1)
    pos = positives.reshape(n_label, 1, q_dev)
    scores, received, info, lse, losses = forward(queries, labels, match, ids, pos)
    partial, label_part, local_sum = backward(scores, received, info, lse, labels, match)
    query_grads, label_grads, rows = scatter(partial, label_part, local_sum)
    matcher_grads = rows.transpose(1, 0, 2, 3).reshape(matcher.shape)
    return (losses[0], query_grads, label_grads, matcher_grads)


def solution(mesh):
    return jax.shard_map(
        body,
        mesh=mesh,
        in_specs=(P(("dp", "label"), None), P("label", None, None), P(), P("dp", None), P("dp")),
        out_specs=(P(("dp", "label")), P(("dp", "label"), None), P("label", "dp", None), P()),
        check_vma=False,
    )
```

```python
import jax
import jax.numpy as jnp
from jax import lax
from jax.experimental import pallas as pl
from jax.experimental.pallas import tpu as pltpu
from jax.sharding import PartitionSpec as P

LEAF = 512
K = 16
BIG = 1e30

MESH = pl.DeviceIdType.MESH

def place():
    me = lax.axis_index("label")
    core = lax.rem(me, 2)
    x = lax.rem(me // 2, 4)
    y = me // 8
    a = x * (1 - core) + y * core
    b = y * (1 - core) + x * core
    return me, core, a, b

def index_of(core, a, b):
    x = a * (1 - core) + b * core
    y = b * (1 - core) + a * core
    return (y * 4 + x) * 2 + core

OFF = (0, 3, 1, 2)

class Links:
    def __init__(self, send, recv):
        self.me, self.core, self.a, self.b = place()
        self.send, self.recv, self.sent = send, recv, []
        c, a, b = self.core, self.a, self.b
        self.partner = self.me + 1 - 2 * c
        self.dev = {
            "a-": index_of(c, lax.rem(a + 3, 4), b),
            "a+": index_of(c, lax.rem(a + 1, 4), b),
            "b-": index_of(c, a, lax.rem(b + 3, 4)),
            "b+": index_of(c, a, lax.rem(b + 1, 4)),
            "p": self.partner,
        }
    def block(self, i, j):
        return index_of(self.core, lax.rem(self.a + OFF[i], 4), lax.rem(self.b + OFF[j], 4))
    def partner_block(self, i, j):
        return index_of(1 - self.core, lax.rem(self.b + OFF[i], 4), lax.rem(self.a + OFF[j], 4))
    def meet(self, peers=None):
        barrier = pltpu.get_barrier_semaphore()
        peers = list(self.dev.values()) if peers is None else peers
        for d in peers:
            pl.semaphore_signal(barrier, inc=1, device_id={"label": d}, device_id_type=MESH)
        pl.semaphore_wait(barrier, len(peers))
    def copy(self, src, dst, slot, to):
        n = len(self.sent)
        c = pltpu.make_async_remote_copy(src_ref=src, dst_ref=dst, send_sem=self.send.at[n],
            recv_sem=self.recv.at[slot], device_id={"label": self.dev[to]}, device_id_type=MESH)
        c.start()
        self.sent.append(c)
    def wait(self, dst, slot):
        pltpu.make_async_remote_copy(src_ref=dst, dst_ref=dst, send_sem=self.send.at[0],
            recv_sem=self.recv.at[slot], device_id={"label": self.partner}, device_id_type=MESH).wait_recv()
    def drain(self):
        for c in self.sent:
            c.wait_send()


SLOTS = 48
TURNS = (
    ((0, 0), (1, 0), (2, 0), (0, 1)),
    ((0, 2), (3, 0), (0, 3), (1, 1)),
    ((1, 2), (2, 1), (2, 2), (1, 3)),
    ((3, 1), (3, 2), (2, 3), (3, 3)),
)


def slot_tables(ids, pos):
    f32 = jnp.float32
    n = ids.shape[1]
    rows = lax.broadcasted_iota(jnp.int32, ids.shape, 0)
    pos_cluster = jnp.sum(
        jnp.where(rows == (pos >> 9), ids, 0).astype(f32), axis=0, keepdims=True
    )
    line = lax.broadcasted_iota(jnp.int32, (8, n), 0)
    named = jnp.zeros((8, n), f32)
    for c in range(4):
        hit = jnp.sum((ids == c).astype(f32), axis=0, keepdims=True)
        named = jnp.where(line == c, hit, named)
    earlier = (
        lax.broadcasted_iota(jnp.int32, (n, n), 0) < lax.broadcasted_iota(jnp.int32, (n, n), 1)
    ).astype(f32)
    rank = jnp.dot(
        named.astype(jnp.bfloat16), earlier.astype(jnp.bfloat16), preferred_element_type=f32
    )
    code = jnp.where(named > 0.5, rank, -1.0)
    target = ((pos & (LEAF - 1)) + 1).astype(f32)
    targets = jnp.where(pos_cluster == (line - 4).astype(f32), target, 0.0)
    return jnp.where(line < 4, code, targets)


def picks(info, c):
    r = lax.broadcasted_iota(jnp.int32, (SLOTS, info.shape[1]), 0).astype(jnp.float32)
    return info[c : c + 1] == r


def target_column(info, pick, c):
    return jnp.sum(jnp.where(pick, info[4 + c : 5 + c], 0.0), axis=1, keepdims=True) - 1.0


def forward_kernel(q_ref, labels, match, ids_ref, pos_ref, scores_out, rec_out, info, lse, losses,
                   g, scores, rec, st, sr, send, recv, st_send, st_recv, lse_send, lse_recv, out_sem):
    f32 = jnp.float32
    L = Links(send, recv)
    peers = [(k, L.block(i, j)) for k, (i, j) in enumerate([(i, j) for i in range(4) for j in range(4)])]
    peers = [d for k, d in peers if k > 0]
    peers += [L.partner_block(i, j) for i in range(4) for j in range(4)]
    L.meet(peers)
    half = q_ref.shape[0] // 2
    first = L.me * 4
    lo = lambda k: g.at[k, pl.ds(0, half)]
    hi = lambda k: g.at[k, pl.ds(half, half)]
    own = L.block(0, 0)
    for to, slot in (("a+", 0), ("a-", 1), ("b+", 4), ("b-", 5), ("p", 20)):
        L.copy(q_ref, g.at[own], slot, to)
    g[own] = q_ref[...]

    def tables(s, carry):
        info[s] = slot_tables(ids_ref[s] - first, pos_ref[s])
        return carry

    lax.fori_loop(0, 32, tables, 0)

    def side_a(i):
        k = L.block(i, 0)
        L.wait(g.at[k], i - 1)
        if i == 1:
            L.copy(lo(k), lo(k), 2, "a+")
        else:
            L.copy(hi(k), hi(k), 3, "a-")
        L.copy(g.at[k], g.at[k], 4 + 4 * i, "b+")
        L.copy(g.at[k], g.at[k], 5 + 4 * i, "b-")
        L.copy(g.at[k], g.at[k], 20 + 4 * i, "p")

    def far_a():
        k = L.block(3, 0)
        L.wait(lo(k), 2)
        L.wait(hi(k), 3)
        L.copy(g.at[k], g.at[k], 16, "b+")
        L.copy(g.at[k], g.at[k], 17, "b-")
        L.copy(g.at[k], g.at[k], 32, "p")

    def side_b(i):
        k = L.block(i, 1)
        L.wait(g.at[k], 4 + 4 * i)
        L.copy(lo(k), lo(k), 6 + 4 * i, "b+")
        L.copy(g.at[k], g.at[k], 21 + 4 * i, "p")
        k = L.block(i, 2)
        L.wait(g.at[k], 5 + 4 * i)
        L.copy(hi(k), hi(k), 7 + 4 * i, "b-")
        L.copy(g.at[k], g.at[k], 22 + 4 * i, "p")

    def far_b(i):
        k = L.block(i, 3)
        L.wait(lo(k), 6 + 4 * i)
        L.wait(hi(k), 7 + 4 * i)
        L.copy(g.at[k], g.at[k], 23 + 4 * i, "p")

    def work(turn, middle):
        members = TURNS[turn]
        for i, j in members:
            L.wait(g.at[L.partner_block(i, j)], 20 + 4 * i + j)
        code_a = sum(OFF[i] << (2 * n) for n, (i, j) in enumerate(members))
        code_b = sum(OFF[j] << (2 * n) for n, (i, j) in enumerate(members))

        def block_of(n):
            other, m = n // 4, lax.rem(n, 4)
            core = L.core + other - 2 * L.core * other
            da = lax.rem(lax.shift_right_logical(jnp.int32(code_a), 2 * m), 4)
            db = lax.rem(lax.shift_right_logical(jnp.int32(code_b), 2 * m), 4)
            a = lax.rem(L.a * (1 - other) + L.b * other + da, 4)
            b = lax.rem(L.b * (1 - other) + L.a * other + db, 4)
            return index_of(core, a, b)

        blocks = [L.block(i, j) for i, j in members] + [L.partner_block(i, j) for i, j in members]

        def pick(n, carry):
            s = block_of(n)
            table = info[s]
            one = jnp.concatenate([picks(table, c).astype(f32) for c in range(4)], axis=0)
            rows = jnp.dot(one.astype(jnp.bfloat16), g[s], preferred_element_type=f32)
            rec[s] = rows.astype(jnp.bfloat16).reshape(4, SLOTS, rows.shape[1])
            return carry

        lax.fori_loop(0, 8, pick, 0)
        middle()

        def score(c, carry):
            rows = jnp.concatenate([rec[k, c] for k in blocks], axis=0)
            out = lax.dot_general(rows, labels[c], (((1,), (1,)), ((), ())), preferred_element_type=f32)
            bias = jnp.sum(rows.astype(f32) * match[c].astype(f32), axis=1, keepdims=True)
            out = out + bias
            for n, k in enumerate(blocks):
                scores[k, c] = out[n * SLOTS : (n + 1) * SLOTS]
            return carry

        lax.fori_loop(0, 4, score, 0)

        def stat(n, carry):
            s = block_of(n)
            table = info[s]
            leaf = lax.broadcasted_iota(jnp.int32, (SLOTS, LEAF), 1).astype(f32)
            parts = []
            for c in range(4):
                one = picks(table, c)
                val = scores[s, c]
                top = jnp.max(val, axis=1, keepdims=True)
                total = jnp.sum(jnp.exp(val - top), axis=1, keepdims=True)
                picked = jnp.sum(
                    jnp.where(leaf == target_column(table, one, c), val, 0.0), axis=1, keepdims=True
                )
                parts.append((one, top, total, picked))
            best = jnp.full((1, table.shape[1]), -BIG, f32)
            for one, top, total, picked in parts:
                best = jnp.maximum(best, jnp.max(jnp.where(one, top, -BIG), axis=0, keepdims=True))
            spread = jnp.zeros_like(best)
            chosen = jnp.zeros_like(best)
            for one, top, total, picked in parts:
                spread += jnp.sum(
                    jnp.where(one, total * jnp.exp(jnp.where(one, top - best, 0.0)), 0.0), axis=0, keepdims=True
                )
                chosen += jnp.sum(jnp.where(one, picked, 0.0), axis=0, keepdims=True)
            line = lax.broadcasted_iota(jnp.int32, (8, table.shape[1]), 0)
            st[s] = jnp.where(line == 0, best, jnp.where(line == 1, spread, chosen))
            return carry

        lax.fori_loop(0, 8, stat, 0)
        for m, k in enumerate(blocks):
            n = 8 * turn + m
            pltpu.make_async_copy(scores.at[k], scores_out.at[k], out_sem.at[2 * n]).start()
            pltpu.make_async_copy(rec.at[k], rec_out.at[k], out_sem.at[2 * n + 1]).start()
            if n == 0:
                continue
            pltpu.make_async_remote_copy(
                src_ref=st.at[k], dst_ref=sr.at[L.me], send_sem=st_send.at[k], recv_sem=st_recv.at[L.me],
                device_id={"label": k}, device_id_type=MESH,
            ).start()
        return blocks

    side_a(1)
    side_a(2)
    side_b(0)
    order = work(0, far_a)
    side_b(1)
    far_b(0)
    order += work(1, lambda: side_b(2))
    far_b(1)
    order += work(2, lambda: side_b(3))
    far_b(2)
    far_b(3)
    order += work(3, lambda: None)
    sr[own] = st[own]

    def stat_copy(k, arrive):
        return pltpu.make_async_remote_copy(
            src_ref=st.at[k], dst_ref=sr.at[k], send_sem=st_send.at[k], recv_sem=st_recv.at[k],
            device_id={"label": k}, device_id_type=MESH,
        )

    for k in peers:
        stat_copy(k, True).wait_recv()
    best = jnp.max(sr[:, 0:1, :], axis=0)
    lines = sr[...]
    spread = jnp.sum(lines[:, 1:2, :] * jnp.exp(lines[:, 0:1, :] - best[None]), axis=0)
    chosen = jnp.sum(lines[:, 2:3, :], axis=0)
    value = best + jnp.log(spread)
    losses[...] = value - chosen
    lse[own] = jnp.broadcast_to(value, lse.shape[1:])

    def lse_copy(dev, row):
        return pltpu.make_async_remote_copy(
            src_ref=lse.at[row], dst_ref=lse.at[row], send_sem=lse_send.at[dev], recv_sem=lse_recv.at[row],
            device_id={"label": dev}, device_id_type=MESH,
        )

    for k in peers:
        lse_copy(k, own).start()
    for k in peers:
        lse_copy(k, k).wait_recv()
    for k in peers:
        stat_copy(k, False).wait_send()
        lse_copy(k, own).wait_send()
    for n, k in enumerate(order):
        pltpu.make_async_copy(scores.at[k], scores_out.at[k], out_sem.at[2 * n]).wait()
        pltpu.make_async_copy(rec.at[k], rec_out.at[k], out_sem.at[2 * n + 1]).wait()
    L.drain()


def forward(q, labels, match, ids, pos):
    q_dev, width = q.shape
    vmem = pl.BlockSpec(memory_space=pltpu.VMEM)
    hbm = pl.BlockSpec(memory_space=pl.ANY)
    shape = jax.ShapeDtypeStruct
    f32, bf16, dma = jnp.float32, jnp.bfloat16, pltpu.SemaphoreType.DMA
    return pl.pallas_call(
        forward_kernel,
        out_shape=(
            shape((32, 4, SLOTS, LEAF), f32),
            shape((32, 4, SLOTS, width), bf16),
            shape((32, 8, q_dev), f32),
            shape((32, 8, q_dev), f32),
            shape((1, q_dev), f32),
        ),
        in_specs=[vmem] * 5,
        out_specs=(hbm, hbm, vmem, vmem, vmem),
        scratch_shapes=[
            pltpu.VMEM((32, q_dev, width), bf16),
            pltpu.VMEM((32, 4, SLOTS, LEAF), f32),
            pltpu.VMEM((32, 4, SLOTS, width), bf16),
            pltpu.VMEM((32, 8, q_dev), f32),
            pltpu.VMEM((32, 8, q_dev), f32),
            dma((36,)), dma((36,)), dma((32,)), dma((32,)), dma((32,)), dma((32,)), dma((64,)),
        ],
        compiler_params=pltpu.CompilerParams(
            collective_id=0, has_side_effects=True, vmem_limit_bytes=60 * 1024 * 1024
        ),
    )(q, labels, match, ids, pos)


def backward_kernel(scores, rec, info, lse, labels, match, partial, label_part, local_sum,
                    delta, coef, grads, held):
    f32, bf16 = jnp.float32, jnp.bfloat16
    step = pl.program_id(0)
    blocks = scores.shape[0]

    @pl.when(step == 0)
    def _():
        local_sum[...] = jnp.zeros_like(local_sum)

    def part(n, carry):
        table = info[n]
        leaf = lax.broadcasted_iota(jnp.int32, (SLOTS, LEAF), 1).astype(f32)
        log_sum = lse[n, 0:1]
        for c in range(4):
            one = picks(table, c)
            used = jnp.sum(jnp.where(one, 1.0, 0.0), axis=1, keepdims=True) > 0.5
            norm = jnp.sum(jnp.where(one, log_sum, 0.0), axis=1, keepdims=True)
            norm = jnp.where(used, norm, BIG)
            hit = leaf == target_column(table, one, c)
            value = jnp.exp(scores[n, c] - norm) - hit.astype(f32)
            total = jnp.sum(value, axis=1, keepdims=True).astype(bf16)
            rows = pl.ds(pl.multiple_of((step * blocks + n) * SLOTS, 16), SLOTS)
            delta[c, rows] = value.astype(bf16)
            coef[c, pl.ds(pl.multiple_of(n * SLOTS, 16), SLOTS)] = jnp.broadcast_to(total.astype(f32), (SLOTS, 128))
            local_sum[c] += jnp.sum(total.astype(f32) * rec[n, c].astype(f32), axis=0, keepdims=True)
        return carry

    lax.fori_loop(0, blocks, part, 0)

    def slot(c, carry):
        rows = pl.ds(pl.multiple_of(step * blocks * SLOTS, 16), blocks * SLOTS)
        out = jnp.dot(delta[c, rows], labels[c], preferred_element_type=f32)
        out = out + coef[c][:, 0:1] * match[c].astype(f32)
        out = out.astype(bf16)
        for n in range(blocks):
            grads[n, pl.ds(pl.multiple_of(c * SLOTS, 16), SLOTS)] = out[n * SLOTS : (n + 1) * SLOTS]
        return carry

    lax.fori_loop(0, 4, slot, 0)

    def back(n, carry):
        table = info[n]
        one = jnp.concatenate([picks(table, c).astype(f32) for c in range(4)], axis=0).astype(bf16)
        out = lax.dot_general(one, grads[n], (((0,), (0,)), ((), ())), preferred_element_type=f32)
        partial[n] = out.astype(bf16)
        return carry

    lax.fori_loop(0, blocks, back, 0)

    for n in range(blocks):
        held[:, pl.ds(pl.multiple_of((step * blocks + n) * SLOTS, 16), SLOTS)] = rec[n]

    @pl.when(step == pl.num_programs(0) - 1)
    def _():
        def gather_part(c, carry):
            out = lax.dot_general(delta[c], held[c], (((0,), (0,)), ((), ())), preferred_element_type=f32)
            label_part[c] = out.astype(bf16)
            return carry

        lax.fori_loop(0, 4, gather_part, 0)


def backward(scores, rec, info, lse, labels, match):
    n, _, _, width = rec.shape
    q_dev = info.shape[2]
    f32, bf16 = jnp.float32, jnp.bfloat16
    group = 8
    vmem = pl.BlockSpec(memory_space=pltpu.VMEM)
    shape = jax.ShapeDtypeStruct
    return pl.pallas_call(
        backward_kernel,
        grid=(n // group,),
        out_shape=(
            shape((n, q_dev, width), bf16),
            shape((4, LEAF, width), bf16),
            shape((4, 1, width), f32),
        ),
        in_specs=[
            pl.BlockSpec((group, 4, SLOTS, LEAF), lambda i: (i, 0, 0, 0)),
            pl.BlockSpec((group, 4, SLOTS, width), lambda i: (i, 0, 0, 0)),
            pl.BlockSpec((group, 8, q_dev), lambda i: (i, 0, 0)),
            pl.BlockSpec((group, 8, q_dev), lambda i: (i, 0, 0)),
            vmem,
            vmem,
        ],
        out_specs=(
            pl.BlockSpec((group, q_dev, width), lambda i: (i, 0, 0)),
            vmem,
            vmem,
        ),
        scratch_shapes=[
            pltpu.VMEM((4, n * SLOTS, LEAF), bf16),
            pltpu.VMEM((4, group * SLOTS, 128), f32),
            pltpu.VMEM((group, 4 * SLOTS, width), bf16),
            pltpu.VMEM((4, n * SLOTS, width), bf16),
        ],
        compiler_params=pltpu.CompilerParams(vmem_limit_bytes=60 * 1024 * 1024),
    )(scores, rec, info, lse, labels, match)


class Column:
    def __init__(self, links):
        self.z = lax.axis_index("dp")
        self.links = links

    def copy(self, src, dst, slot, off):
        L = self.links
        n = len(L.sent)
        c = pltpu.make_async_remote_copy(
            src_ref=src, dst_ref=dst, send_sem=L.send.at[n], recv_sem=L.recv.at[slot],
            device_id={"dp": lax.rem(self.z + off, 4)}, device_id_type=MESH,
        )
        c.start()
        L.sent.append(c)


def scatter_kernel(p, lp, ls, out, label_out, mout, t_all, u, pr, bh, bf, ah, af, zt, zh, zf, mz, send, recv, m_recv):
    L = Links(send, recv)
    Z = Column(L)
    z = Z.z
    peers = [L.block(i, j) for i in range(4) for j in range(4)][1:]
    peers += [L.partner_block(i, j) for i in range(4) for j in range(4)]
    barrier = pltpu.get_barrier_semaphore()
    for d in peers:
        pl.semaphore_signal(barrier, inc=1, device_id={"label": d}, device_id_type=MESH)
    for off in (1, 2, 3):
        pl.semaphore_signal(barrier, inc=1, device_id={"dp": lax.rem(z + off, 4)}, device_id_type=MESH)
    pl.semaphore_wait(barrier, 34)
    half = p.shape[1] // 2
    f32 = jnp.float32
    rows_z = label_out.shape[1]

    def rows(off):
        return pl.ds(pl.multiple_of(lax.rem(z + off, 4) * rows_z, rows_z), rows_z)

    PAIRS = pl.ds(0, 2), pl.ds(2, 2)
    for off in (1, 2, 3):
        Z.copy(ls.at[lax.rem(z + off, 4)], mz.at[z], 41 + off, off)
    ORDER = [(i, 3) for i in (3, 1, 2, 0)] + [(i, j) for i in (3, 1, 2, 0) for j in (1, 2)] + [(i, 0) for i in (3, 1, 2, 0)]
    for i, j in ORDER:
        L.copy(p.at[L.partner_block(i, j)], pr.at[4 * i + j], 4 * i + j, "p")
    Z.copy(lp.at[PAIRS[0], rows(2)], zh.at[0], 36, 1)
    Z.copy(lp.at[PAIRS[1], rows(2)], zh.at[1], 37, 3)
    LO, HI = pl.ds(0, half), pl.ds(half, half)
    mz[z] = ls[z]

    def both(i, j):
        L.wait(pr.at[4 * i + j], 4 * i + j)
        return lambda s: p[L.block(i, j), s].astype(f32) + pr[4 * i + j, s].astype(f32)

    for i in (3, 1, 2, 0):
        s = both(i, 3)
        t = t_all.at[3 * i + 2]
        t[...] = s(slice(None)).astype(t.dtype)
        L.copy(t.at[LO], bh.at[i, 0], 16 + 4 * i, "b+")
        L.copy(t.at[HI], bh.at[i, 1], 17 + 4 * i, "b-")
    for off in (1, 2, 3):
        L.wait(mz.at[lax.rem(z + 4 - off, 4)], 41 + off)
    mout[z, L.me] = mz[0] + mz[1] + mz[2] + mz[3]

    def row_copy(dev, row):
        return pltpu.make_async_remote_copy(
            src_ref=mout.at[z, row], dst_ref=mout.at[z, row], send_sem=m_recv.at[1, dev], recv_sem=m_recv.at[0, row],
            device_id={"label": dev}, device_id_type=MESH,
        )

    for k in peers:
        row_copy(k, L.me).start()
    L.wait(zh.at[0], 36)
    zt[1, 0:2] = (lp[PAIRS[0], rows(1)].astype(f32) + zh[0].astype(f32)).astype(zt.dtype)
    zt[1, 2:4] = lp[PAIRS[1], rows(1)]
    Z.copy(zt.at[1], zf.at[0], 38, 1)
    L.wait(zh.at[1], 37)
    zt[0, 2:4] = (lp[PAIRS[1], rows(3)].astype(f32) + zh[1].astype(f32)).astype(zt.dtype)
    zt[0, 0:2] = lp[PAIRS[0], rows(3)]
    Z.copy(zt.at[0], zf.at[1], 39, 3)
    for i in (3, 1, 2, 0):
        s = both(i, 2)
        t = t_all.at[3 * i + 1]
        L.wait(bh.at[i, 0], 16 + 4 * i)
        t[LO] = (s(LO) + bh[i, 0].astype(f32)).astype(t.dtype)
        t[HI] = s(HI).astype(t.dtype)
        L.copy(t, bf.at[i, 0], 18 + 4 * i, "b+")
        s = both(i, 1)
        t = t_all.at[3 * i + 0]
        L.wait(bh.at[i, 1], 17 + 4 * i)
        t[HI] = (s(HI) + bh[i, 1].astype(f32)).astype(t.dtype)
        t[LO] = s(LO).astype(t.dtype)
        L.copy(t, bf.at[i, 1], 19 + 4 * i, "b-")
    for k in peers:
        row_copy(k, k).wait_recv()
    for off in (1, 2, 3):
        Z.copy(mout.at[z], mout.at[z], 44 + off, off)

    def column(i):
        s = both(i, 0)
        L.wait(bf.at[i, 0], 18 + 4 * i)
        L.wait(bf.at[i, 1], 19 + 4 * i)
        return lambda r: s(r) + bf[i, 0, r].astype(f32) + bf[i, 1, r].astype(f32)

    s = column(3)
    u[2] = s(slice(None)).astype(u.dtype)
    L.copy(u.at[2, LO], ah.at[0], 32, "a+")
    L.copy(u.at[2, HI], ah.at[1], 33, "a-")
    s = column(1)
    L.wait(ah.at[1], 33)
    u[0, HI] = (s(HI) + ah[1].astype(f32)).astype(u.dtype)
    u[0, LO] = s(LO).astype(u.dtype)
    L.copy(u.at[0], af.at[1], 35, "a-")
    s = column(2)
    L.wait(ah.at[0], 32)
    u[1, LO] = (s(LO) + ah[0].astype(f32)).astype(u.dtype)
    u[1, HI] = s(HI).astype(u.dtype)
    L.copy(u.at[1], af.at[0], 34, "a+")
    L.wait(zf.at[0], 38)
    L.wait(zf.at[1], 39)
    label_out[...] = lp[:, rows(0)].astype(f32) + zf[0].astype(f32) + zf[1].astype(f32)
    s = column(0)
    L.wait(af.at[0], 34)
    L.wait(af.at[1], 35)
    out[...] = s(slice(None)) + af[0].astype(f32) + af[1].astype(f32)
    for off in (1, 2, 3):
        L.wait(mout.at[lax.rem(z + 4 - off, 4)], 44 + off)
    for k in peers:
        row_copy(k, L.me).wait_send()
    L.drain()


def scatter(p, lp, ls):
    n, r, w = p.shape
    clusters, leaf, _ = lp.shape
    f32, bf16, dma = jnp.float32, jnp.bfloat16, pltpu.SemaphoreType.DMA
    vmem = pl.BlockSpec(memory_space=pltpu.VMEM)
    shape = jax.ShapeDtypeStruct
    return pl.pallas_call(
        scatter_kernel,
        out_shape=(shape((r, w), f32), shape((clusters, leaf // 4, w), f32), shape((4, n, 1, w), f32)),
        in_specs=[vmem] * 3,
        out_specs=(vmem,) * 3,
        scratch_shapes=[
            pltpu.VMEM((12, r, w), bf16),
            pltpu.VMEM((3, r, w), bf16),
            pltpu.VMEM((16, r, w), bf16),
            pltpu.VMEM((4, 2, r // 2, w), bf16),
            pltpu.VMEM((4, 2, r, w), bf16),
            pltpu.VMEM((2, r // 2, w), bf16),
            pltpu.VMEM((2, r, w), bf16),
            pltpu.VMEM((2, clusters, leaf // 4, w), bf16),
            pltpu.VMEM((2, 2, leaf // 4, w), bf16),
            pltpu.VMEM((2, clusters, leaf // 4, w), bf16),
            pltpu.VMEM((4, 1, w), f32),
            dma((52,)),
            dma((48,)),
            dma((2, 32)),
        ],
        compiler_params=pltpu.CompilerParams(
            collective_id=1, has_side_effects=True, vmem_limit_bytes=60 * 1024 * 1024
        ),
    )(p, lp, ls)


def body(queries, labels, matcher, cluster_ids, positives):
    q_dev, width = queries.shape
    cl_dev = labels.shape[0]
    n_label = lax.axis_size("label")
    first = lax.axis_index("label") * cl_dev
    match = lax.dynamic_slice_in_dim(matcher, first, cl_dev, 0).reshape(cl_dev, 1, width)
    ids = cluster_ids.reshape(n_label, q_dev, K).transpose(0, 2, 1)
    pos = positives.reshape(n_label, 1, q_dev)
    scores, received, info, lse, losses = forward(queries, labels, match, ids, pos)
    partial, label_part, local_sum = backward(scores, received, info, lse, labels, match)
    query_grads, label_grads, rows = scatter(partial, label_part, local_sum)
    matcher_grads = rows.transpose(1, 0, 2, 3).reshape(matcher.shape)
    return (losses.reshape(q_dev), query_grads, label_grads, matcher_grads)


def solution(mesh):
    return jax.shard_map(
        body,
        mesh=mesh,
        in_specs=(P(("dp", "label"), None), P("label", None, None), P(), P("dp", None), P("dp")),
        out_specs=(P(("dp", "label")), P(("dp", "label"), None), P("label", "dp", None), P()),
        check_vma=False,
    )
```

```python
import jax
import jax.numpy as jnp
from jax import lax
from jax.experimental import pallas as pl
from jax.experimental.pallas import tpu as pltpu
from jax.sharding import PartitionSpec as P

LEAF = 512
K = 16
BIG = 1e30

MESH = pl.DeviceIdType.MESH

def place():
    me = lax.axis_index("label")
    core = lax.rem(me, 2)
    x = lax.rem(me // 2, 4)
    y = me // 8
    a = x * (1 - core) + y * core
    b = y * (1 - core) + x * core
    return me, core, a, b

def index_of(core, a, b):
    x = a * (1 - core) + b * core
    y = b * (1 - core) + a * core
    return (y * 4 + x) * 2 + core

OFF = (0, 3, 1, 2)

class Links:
    def __init__(self, send, recv):
        self.me, self.core, self.a, self.b = place()
        self.send, self.recv, self.sent = send, recv, []
        c, a, b = self.core, self.a, self.b
        self.partner = self.me + 1 - 2 * c
        self.dev = {
            "a-": index_of(c, lax.rem(a + 3, 4), b),
            "a+": index_of(c, lax.rem(a + 1, 4), b),
            "b-": index_of(c, a, lax.rem(b + 3, 4)),
            "b+": index_of(c, a, lax.rem(b + 1, 4)),
            "p": self.partner,
        }
    def block(self, i, j):
        return index_of(self.core, lax.rem(self.a + OFF[i], 4), lax.rem(self.b + OFF[j], 4))
    def partner_block(self, i, j):
        return index_of(1 - self.core, lax.rem(self.b + OFF[i], 4), lax.rem(self.a + OFF[j], 4))
    def meet(self, peers=None):
        barrier = pltpu.get_barrier_semaphore()
        peers = list(self.dev.values()) if peers is None else peers
        for d in peers:
            pl.semaphore_signal(barrier, inc=1, device_id={"label": d}, device_id_type=MESH)
        pl.semaphore_wait(barrier, len(peers))
    def copy(self, src, dst, slot, to):
        n = len(self.sent)
        c = pltpu.make_async_remote_copy(src_ref=src, dst_ref=dst, send_sem=self.send.at[n],
            recv_sem=self.recv.at[slot], device_id={"label": self.dev[to]}, device_id_type=MESH)
        c.start()
        self.sent.append(c)
    def wait(self, dst, slot):
        pltpu.make_async_remote_copy(src_ref=dst, dst_ref=dst, send_sem=self.send.at[0],
            recv_sem=self.recv.at[slot], device_id={"label": self.partner}, device_id_type=MESH).wait_recv()
    def drain(self):
        for c in self.sent:
            c.wait_send()


SLOTS = 48
TURNS = (
    ((0, 0), (1, 0), (2, 0), (0, 1)),
    ((0, 2), (3, 0), (0, 3), (1, 1)),
    ((1, 2), (2, 1), (2, 2), (1, 3)),
    ((3, 1), (3, 2), (2, 3), (3, 3)),
)


def slot_tables(ids, pos):
    f32 = jnp.float32
    n = ids.shape[1]
    rows = lax.broadcasted_iota(jnp.int32, ids.shape, 0)
    pos_cluster = jnp.sum(
        jnp.where(rows == (pos >> 9), ids, 0).astype(f32), axis=0, keepdims=True
    )
    line = lax.broadcasted_iota(jnp.int32, (8, n), 0)
    named = jnp.zeros((8, n), f32)
    for c in range(4):
        hit = jnp.sum((ids == c).astype(f32), axis=0, keepdims=True)
        named = jnp.where(line == c, hit, named)
    earlier = (
        lax.broadcasted_iota(jnp.int32, (n, n), 0) < lax.broadcasted_iota(jnp.int32, (n, n), 1)
    ).astype(f32)
    rank = jnp.dot(
        named.astype(jnp.bfloat16), earlier.astype(jnp.bfloat16), preferred_element_type=f32
    )
    code = jnp.where(named > 0.5, rank, -1.0)
    target = ((pos & (LEAF - 1)) + 1).astype(f32)
    targets = jnp.where(pos_cluster == (line - 4).astype(f32), target, 0.0)
    return jnp.where(line < 4, code, targets)


def picks(info, c):
    r = lax.broadcasted_iota(jnp.int32, (SLOTS, info.shape[1]), 0).astype(jnp.float32)
    return info[c : c + 1] == r


def target_column(info, pick, c):
    return jnp.sum(jnp.where(pick, info[4 + c : 5 + c], 0.0), axis=1, keepdims=True) - 1.0


def forward_kernel(q_ref, labels, match, ids_ref, pos_ref, scores_out, rec_out, info, lse, losses,
                   g, scores, rec, st, sr, send, recv, st_send, st_recv, lse_send, lse_recv, out_sem):
    f32 = jnp.float32
    L = Links(send, recv)
    peers = [(k, L.block(i, j)) for k, (i, j) in enumerate([(i, j) for i in range(4) for j in range(4)])]
    peers = [d for k, d in peers if k > 0]
    peers += [L.partner_block(i, j) for i in range(4) for j in range(4)]
    L.meet(peers)
    half = q_ref.shape[0] // 2
    first = L.me * 4
    lo = lambda k: g.at[k, pl.ds(0, half)]
    hi = lambda k: g.at[k, pl.ds(half, half)]
    own = L.block(0, 0)
    for to, slot in (("a+", 0), ("a-", 1), ("b+", 4), ("b-", 5), ("p", 20)):
        L.copy(q_ref, g.at[own], slot, to)
    g[own] = q_ref[...]

    def tables(s, carry):
        info[s] = slot_tables(ids_ref[s] - first, pos_ref[s])
        return carry

    lax.fori_loop(0, 32, tables, 0)

    def side_a(i):
        k = L.block(i, 0)
        L.wait(g.at[k], i - 1)
        if i == 1:
            L.copy(lo(k), lo(k), 2, "a+")
        else:
            L.copy(hi(k), hi(k), 3, "a-")
        L.copy(g.at[k], g.at[k], 4 + 4 * i, "b+")
        L.copy(g.at[k], g.at[k], 5 + 4 * i, "b-")
        L.copy(g.at[k], g.at[k], 20 + 4 * i, "p")

    def far_a():
        k = L.block(3, 0)
        L.wait(lo(k), 2)
        L.wait(hi(k), 3)
        L.copy(g.at[k], g.at[k], 16, "b+")
        L.copy(g.at[k], g.at[k], 17, "b-")
        L.copy(g.at[k], g.at[k], 32, "p")

    def side_b(i):
        k = L.block(i, 1)
        L.wait(g.at[k], 4 + 4 * i)
        L.copy(lo(k), lo(k), 6 + 4 * i, "b+")
        L.copy(g.at[k], g.at[k], 21 + 4 * i, "p")
        k = L.block(i, 2)
        L.wait(g.at[k], 5 + 4 * i)
        L.copy(hi(k), hi(k), 7 + 4 * i, "b-")
        L.copy(g.at[k], g.at[k], 22 + 4 * i, "p")

    def far_b(i):
        k = L.block(i, 3)
        L.wait(lo(k), 6 + 4 * i)
        L.wait(hi(k), 7 + 4 * i)
        L.copy(g.at[k], g.at[k], 23 + 4 * i, "p")

    def work(turn, middle):
        members = TURNS[turn]
        for i, j in members:
            L.wait(g.at[L.partner_block(i, j)], 20 + 4 * i + j)
        code_a = sum(OFF[i] << (2 * n) for n, (i, j) in enumerate(members))
        code_b = sum(OFF[j] << (2 * n) for n, (i, j) in enumerate(members))

        def block_of(n):
            other, m = n // 4, lax.rem(n, 4)
            core = L.core + other - 2 * L.core * other
            da = lax.rem(lax.shift_right_logical(jnp.int32(code_a), 2 * m), 4)
            db = lax.rem(lax.shift_right_logical(jnp.int32(code_b), 2 * m), 4)
            a = lax.rem(L.a * (1 - other) + L.b * other + da, 4)
            b = lax.rem(L.b * (1 - other) + L.a * other + db, 4)
            return index_of(core, a, b)

        blocks = [L.block(i, j) for i, j in members] + [L.partner_block(i, j) for i, j in members]

        def pick(n, carry):
            s = block_of(n)
            table = info[s]
            one = jnp.concatenate([picks(table, c).astype(f32) for c in range(4)], axis=0)
            rows = jnp.dot(one.astype(jnp.bfloat16), g[s], preferred_element_type=f32)
            rec[s] = rows.astype(jnp.bfloat16).reshape(4, SLOTS, rows.shape[1])
            return carry

        lax.fori_loop(0, 8, pick, 0)
        middle()

        def score(c, carry):
            rows = jnp.concatenate([rec[k, c] for k in blocks], axis=0)
            out = lax.dot_general(rows, labels[c], (((1,), (1,)), ((), ())), preferred_element_type=f32)
            bias = jnp.sum(rows.astype(f32) * match[c].astype(f32), axis=1, keepdims=True)
            out = out + bias
            for n, k in enumerate(blocks):
                scores[k, c] = out[n * SLOTS : (n + 1) * SLOTS]
            return carry

        lax.fori_loop(0, 4, score, 0)

        def stat(n, carry):
            s = block_of(n)
            table = info[s]
            leaf = lax.broadcasted_iota(jnp.int32, (SLOTS, LEAF), 1).astype(f32)
            parts = []
            for c in range(4):
                one = picks(table, c)
                val = scores[s, c]
                top = jnp.max(val, axis=1, keepdims=True)
                total = jnp.sum(jnp.exp(val - top), axis=1, keepdims=True)
                picked = jnp.sum(
                    jnp.where(leaf == target_column(table, one, c), val, 0.0), axis=1, keepdims=True
                )
                parts.append((one, top, total, picked))
            best = jnp.full((1, table.shape[1]), -BIG, f32)
            for one, top, total, picked in parts:
                best = jnp.maximum(best, jnp.max(jnp.where(one, top, -BIG), axis=0, keepdims=True))
            spread = jnp.zeros_like(best)
            chosen = jnp.zeros_like(best)
            for one, top, total, picked in parts:
                spread += jnp.sum(
                    jnp.where(one, total * jnp.exp(jnp.where(one, top - best, 0.0)), 0.0), axis=0, keepdims=True
                )
                chosen += jnp.sum(jnp.where(one, picked, 0.0), axis=0, keepdims=True)
            line = lax.broadcasted_iota(jnp.int32, (8, table.shape[1]), 0)
            st[s] = jnp.where(line == 0, best, jnp.where(line == 1, spread, chosen))
            return carry

        lax.fori_loop(0, 8, stat, 0)
        for m, k in enumerate(blocks):
            n = 8 * turn + m
            pltpu.make_async_copy(scores.at[k], scores_out.at[k], out_sem.at[2 * n]).start()
            pltpu.make_async_copy(rec.at[k], rec_out.at[k], out_sem.at[2 * n + 1]).start()
            if n == 0:
                continue
            pltpu.make_async_remote_copy(
                src_ref=st.at[k], dst_ref=sr.at[L.me], send_sem=st_send.at[k], recv_sem=st_recv.at[L.me],
                device_id={"label": k}, device_id_type=MESH,
            ).start()
        return blocks

    side_a(1)
    side_a(2)
    side_b(0)
    order = work(0, far_a)
    side_b(1)
    far_b(0)
    order += work(1, lambda: side_b(2))
    far_b(1)
    order += work(2, lambda: side_b(3))
    far_b(2)
    far_b(3)
    order += work(3, lambda: None)
    sr[own] = st[own]

    def stat_copy(k, arrive):
        return pltpu.make_async_remote_copy(
            src_ref=st.at[k], dst_ref=sr.at[k], send_sem=st_send.at[k], recv_sem=st_recv.at[k],
            device_id={"label": k}, device_id_type=MESH,
        )

    for k in peers:
        stat_copy(k, True).wait_recv()
    best = jnp.max(sr[:, 0:1, :], axis=0)
    lines = sr[...]
    spread = jnp.sum(lines[:, 1:2, :] * jnp.exp(lines[:, 0:1, :] - best[None]), axis=0)
    chosen = jnp.sum(lines[:, 2:3, :], axis=0)
    value = best + jnp.log(spread)
    losses[...] = value - chosen
    lse[own] = jnp.broadcast_to(value, lse.shape[1:])

    def lse_copy(dev, row):
        return pltpu.make_async_remote_copy(
            src_ref=lse.at[row], dst_ref=lse.at[row], send_sem=lse_send.at[dev], recv_sem=lse_recv.at[row],
            device_id={"label": dev}, device_id_type=MESH,
        )

    for k in peers:
        lse_copy(k, own).start()
    for k in peers:
        lse_copy(k, k).wait_recv()
    for k in peers:
        stat_copy(k, False).wait_send()
        lse_copy(k, own).wait_send()
    for n, k in enumerate(order):
        pltpu.make_async_copy(scores.at[k], scores_out.at[k], out_sem.at[2 * n]).wait()
        pltpu.make_async_copy(rec.at[k], rec_out.at[k], out_sem.at[2 * n + 1]).wait()
    L.drain()


def forward(q, labels, match, ids, pos):
    q_dev, width = q.shape
    vmem = pl.BlockSpec(memory_space=pltpu.VMEM)
    hbm = pl.BlockSpec(memory_space=pl.ANY)
    shape = jax.ShapeDtypeStruct
    f32, bf16, dma = jnp.float32, jnp.bfloat16, pltpu.SemaphoreType.DMA
    return pl.pallas_call(
        forward_kernel,
        out_shape=(
            shape((32, 4, SLOTS, LEAF), f32),
            shape((32, 4, SLOTS, width), bf16),
            shape((32, 8, q_dev), f32),
            shape((32, 8, q_dev), f32),
            shape((1, q_dev), f32),
        ),
        in_specs=[vmem] * 5,
        out_specs=(hbm, hbm, vmem, vmem, vmem),
        scratch_shapes=[
            pltpu.VMEM((32, q_dev, width), bf16),
            pltpu.VMEM((32, 4, SLOTS, LEAF), f32),
            pltpu.VMEM((32, 4, SLOTS, width), bf16),
            pltpu.VMEM((32, 8, q_dev), f32),
            pltpu.VMEM((32, 8, q_dev), f32),
            dma((36,)), dma((36,)), dma((32,)), dma((32,)), dma((32,)), dma((32,)), dma((64,)),
        ],
        compiler_params=pltpu.CompilerParams(
            collective_id=0, has_side_effects=True, vmem_limit_bytes=60 * 1024 * 1024
        ),
    )(q, labels, match, ids, pos)


class Column:
    def __init__(self, links):
        self.z = lax.axis_index("dp")
        self.links = links

    def copy(self, src, dst, slot, off):
        L = self.links
        n = len(L.sent)
        c = pltpu.make_async_remote_copy(
            src_ref=src, dst_ref=dst, send_sem=L.send.at[n], recv_sem=L.recv.at[slot],
            device_id={"dp": lax.rem(self.z + off, 4)}, device_id_type=MESH,
        )
        c.start()
        L.sent.append(c)


BACK_TURNS = (
    ((3, 3), (1, 3), (2, 3), (0, 3)),
    ((3, 1), (3, 2), (1, 1), (1, 2)),
    ((2, 1), (2, 2), (0, 1), (0, 2)),
    ((3, 0), (1, 0), (2, 0), (0, 0)),
)


def backward_kernel(labels, match, info, lse, scores_hbm, rec_hbm, out, label_out, mout,
                    stage, rec, delta, coef, grads, p, lp, ls, pr, bh, bf, ah, af, zt, zh, zf, mz,
                    send, recv, m_recv, in_sem):
    L = Links(send, recv)
    Z = Column(L)
    z = Z.z
    f32, bf16 = jnp.float32, jnp.bfloat16
    turns = [
        [L.block(i, j) for i, j in t] + [L.partner_block(i, j) for i, j in t] for t in BACK_TURNS
    ]

    def load_scores(t):
        return [
            pltpu.make_async_copy(scores_hbm.at[k], stage.at[t % 2, m], in_sem.at[0, 8 * t + m])
            for m, k in enumerate(turns[t])
        ]

    def load_rows(t):
        return [
            pltpu.make_async_copy(rec_hbm.at[k], rec.at[k], in_sem.at[1, 8 * t + m])
            for m, k in enumerate(turns[t])
        ]

    for t in range(2):
        for c in load_scores(t) + load_rows(t):
            c.start()
    for t in range(2, 4):
        for c in load_rows(t):
            c.start()
    peers = [L.block(i, j) for i in range(4) for j in range(4)][1:]
    peers += [L.partner_block(i, j) for i in range(4) for j in range(4)]
    barrier = pltpu.get_barrier_semaphore()
    for d in peers:
        pl.semaphore_signal(barrier, inc=1, device_id={"label": d}, device_id_type=MESH)
    for off in (1, 2, 3):
        pl.semaphore_signal(barrier, inc=1, device_id={"dp": lax.rem(z + off, 4)}, device_id_type=MESH)
    ls[...] = jnp.zeros_like(ls)

    def block_of(t, n):
        code_a = sum(OFF[i] << (2 * m) for m, (i, j) in enumerate(BACK_TURNS[t]))
        code_b = sum(OFF[j] << (2 * m) for m, (i, j) in enumerate(BACK_TURNS[t]))
        other, m = n // 4, lax.rem(n, 4)
        core = L.core + other - 2 * L.core * other
        da = lax.rem(lax.shift_right_logical(jnp.int32(code_a), 2 * m), 4)
        db = lax.rem(lax.shift_right_logical(jnp.int32(code_b), 2 * m), 4)
        a = lax.rem(L.a * (1 - other) + L.b * other + da, 4)
        b = lax.rem(L.b * (1 - other) + L.a * other + db, 4)
        return index_of(core, a, b)

    def part(t):
        for c in load_scores(t) + load_rows(t):
            c.wait()

        def step(n, carry):
            k = block_of(t, n)
            table = info[k]
            leaf = lax.broadcasted_iota(jnp.int32, (SLOTS, LEAF), 1).astype(f32)
            log_sum = lse[k, 0:1]
            for c in range(4):
                one = picks(table, c)
                used = jnp.sum(jnp.where(one, 1.0, 0.0), axis=1, keepdims=True) > 0.5
                norm = jnp.sum(jnp.where(one, log_sum, 0.0), axis=1, keepdims=True)
                norm = jnp.where(used, norm, BIG)
                hit = leaf == target_column(table, one, c)
                value = jnp.exp(stage[t % 2, n, c] - norm) - hit.astype(f32)
                total = jnp.sum(value, axis=1, keepdims=True).astype(bf16)
                delta[k, c] = value.astype(bf16)
                coef[k, c] = jnp.broadcast_to(total.astype(f32), (SLOTS, 128)).astype(bf16)
                ls[c] += jnp.sum(total.astype(f32) * rec[k, c].astype(f32), axis=0, keepdims=True)
            return carry

        lax.fori_loop(0, 8, step, 0)
        if t < 2:
            for c in load_scores(t + 2):
                c.start()

    def slots(t):
        def slot(c, carry):
            rows = jnp.concatenate([delta[k, c] for k in turns[t]], axis=0)
            scale = jnp.concatenate([coef[k, c] for k in turns[t]], axis=0)[:, 0:1].astype(f32)
            val = jnp.dot(rows, labels[c], preferred_element_type=f32)
            val = (val + scale * match[c].astype(f32)).astype(bf16)
            for n in range(8):
                grads[n, pl.ds(pl.multiple_of(c * SLOTS, 16), SLOTS)] = val[n * SLOTS : (n + 1) * SLOTS]
            return carry

        lax.fori_loop(0, 4, slot, 0)

        def back(n, carry):
            k = block_of(t, n)
            table = info[k]
            one = jnp.concatenate([picks(table, c).astype(f32) for c in range(4)], axis=0).astype(bf16)
            val = lax.dot_general(one, grads[n], (((0,), (0,)), ((), ())), preferred_element_type=f32)
            p[k] = val.astype(bf16)
            return carry

        lax.fori_loop(0, 8, back, 0)
        for i, j in BACK_TURNS[t]:
            L.copy(p.at[L.partner_block(i, j)], pr.at[4 * i + j], 4 * i + j, "p")

    def label_parts(low):
        def one_part(c, carry):
            left = jnp.concatenate([delta[k, c] for k in range(32)], axis=0)
            right = jnp.concatenate([rec[k, c] for k in range(32)], axis=0)
            val = lax.dot_general(left, right, (((0,), (0,)), ((), ())), preferred_element_type=f32)
            lp[c] = val.astype(bf16)
            return carry

        lax.fori_loop(low, low + 2, one_part, 0)

    half = p.shape[1] // 2
    rows_z = label_out.shape[1]

    def rows(off):
        return pl.ds(pl.multiple_of(lax.rem(z + off, 4) * rows_z, rows_z), rows_z)

    PAIRS = pl.ds(0, 2), pl.ds(2, 2)
    LO, HI = pl.ds(0, half), pl.ds(half, half)

    def both(i, j):
        L.wait(pr.at[4 * i + j], 4 * i + j)
        return lambda s: p[L.block(i, j), s].astype(f32) + pr[4 * i + j, s].astype(f32)

    def far(i):
        s = both(i, 3)
        t = p.at[L.block(i, 3)]
        t[...] = s(slice(None)).astype(t.dtype)
        L.copy(t.at[LO], bh.at[i, 0], 16 + 4 * i, "b+")
        L.copy(t.at[HI], bh.at[i, 1], 17 + 4 * i, "b-")

    def near(i):
        s = both(i, 2)
        t = p.at[L.block(i, 2)]
        L.wait(bh.at[i, 0], 16 + 4 * i)
        t[LO] = (s(LO) + bh[i, 0].astype(f32)).astype(t.dtype)
        t[HI] = s(HI).astype(t.dtype)
        L.copy(t, bf.at[i, 0], 18 + 4 * i, "b+")
        s = both(i, 1)
        t = p.at[L.block(i, 1)]
        L.wait(bh.at[i, 1], 17 + 4 * i)
        t[HI] = (s(HI) + bh[i, 1].astype(f32)).astype(t.dtype)
        t[LO] = s(LO).astype(t.dtype)
        L.copy(t, bf.at[i, 1], 19 + 4 * i, "b-")

    def column(i):
        s = both(i, 0)
        L.wait(bf.at[i, 0], 18 + 4 * i)
        L.wait(bf.at[i, 1], 19 + 4 * i)
        return lambda r: s(r) + bf[i, 0, r].astype(f32) + bf[i, 1, r].astype(f32)

    def row_copy(dev, row):
        return pltpu.make_async_remote_copy(
            src_ref=mout.at[z, row], dst_ref=mout.at[z, row], send_sem=m_recv.at[1, dev], recv_sem=m_recv.at[0, row],
            device_id={"label": dev}, device_id_type=MESH,
        )

    part(0)
    pl.semaphore_wait(barrier, 34)
    slots(0)
    part(1)
    for i in (3, 1, 2, 0):
        far(i)
    part(2)
    part(3)
    mz[z] = ls[z]
    for off in (1, 2, 3):
        Z.copy(ls.at[lax.rem(z + off, 4)], mz.at[z], 41 + off, off)
    slots(1)
    label_parts(0)
    Z.copy(lp.at[PAIRS[0], rows(2)], zh.at[0], 36, 1)
    near(3)
    near(1)
    label_parts(2)
    Z.copy(lp.at[PAIRS[1], rows(2)], zh.at[1], 37, 3)
    for off in (1, 2, 3):
        L.wait(mz.at[lax.rem(z + 4 - off, 4)], 41 + off)
    mout[z, L.me] = mz[0] + mz[1] + mz[2] + mz[3]
    for k in peers:
        row_copy(k, L.me).start()
    slots(2)
    L.wait(zh.at[0], 36)
    zt[1, 0:2] = (lp[PAIRS[0], rows(1)].astype(f32) + zh[0].astype(f32)).astype(zt.dtype)
    zt[1, 2:4] = lp[PAIRS[1], rows(1)]
    Z.copy(zt.at[1], zf.at[0], 38, 1)
    near(2)
    near(0)
    L.wait(zh.at[1], 37)
    zt[0, 2:4] = (lp[PAIRS[1], rows(3)].astype(f32) + zh[1].astype(f32)).astype(zt.dtype)
    zt[0, 0:2] = lp[PAIRS[0], rows(3)]
    Z.copy(zt.at[0], zf.at[1], 39, 3)
    slots(3)
    for k in peers:
        row_copy(k, k).wait_recv()
    for off in (1, 2, 3):
        Z.copy(mout.at[z], mout.at[z], 44 + off, off)
    s = column(3)
    u = p.at[L.block(3, 0)]
    u[...] = s(slice(None)).astype(u.dtype)
    L.copy(u.at[LO], ah.at[0], 32, "a+")
    L.copy(u.at[HI], ah.at[1], 33, "a-")
    s = column(1)
    u = p.at[L.block(1, 0)]
    L.wait(ah.at[1], 33)
    u[HI] = (s(HI) + ah[1].astype(f32)).astype(u.dtype)
    u[LO] = s(LO).astype(u.dtype)
    L.copy(u, af.at[1], 35, "a-")
    s = column(2)
    u = p.at[L.block(2, 0)]
    L.wait(ah.at[0], 32)
    u[LO] = (s(LO) + ah[0].astype(f32)).astype(u.dtype)
    u[HI] = s(HI).astype(u.dtype)
    L.copy(u, af.at[0], 34, "a+")
    L.wait(zf.at[0], 38)
    L.wait(zf.at[1], 39)
    label_out[...] = lp[:, rows(0)].astype(f32) + zf[0].astype(f32) + zf[1].astype(f32)
    s = column(0)
    L.wait(af.at[0], 34)
    L.wait(af.at[1], 35)
    out[...] = s(slice(None)) + af[0].astype(f32) + af[1].astype(f32)
    for off in (1, 2, 3):
        L.wait(mout.at[lax.rem(z + 4 - off, 4)], 44 + off)
    for k in peers:
        row_copy(k, L.me).wait_send()
    L.drain()


def backward(labels, match, info, lse, scores, rec):
    n, _, r = info.shape
    clusters, leaf, w = labels.shape
    f32, bf16, dma = jnp.float32, jnp.bfloat16, pltpu.SemaphoreType.DMA
    vmem = pl.BlockSpec(memory_space=pltpu.VMEM)
    hbm = pl.BlockSpec(memory_space=pl.ANY)
    shape = jax.ShapeDtypeStruct
    return pl.pallas_call(
        backward_kernel,
        out_shape=(shape((r, w), f32), shape((clusters, leaf // 4, w), f32), shape((4, n, 1, w), f32)),
        in_specs=[vmem] * 4 + [hbm] * 2,
        out_specs=(vmem,) * 3,
        scratch_shapes=[
            pltpu.VMEM((2, 8, 4, SLOTS, leaf), f32),
            pltpu.VMEM((n, 4, SLOTS, w), bf16),
            pltpu.VMEM((n, 4, SLOTS, leaf), bf16),
            pltpu.VMEM((n, 4, SLOTS, 128), bf16),
            pltpu.VMEM((8, 4 * SLOTS, w), bf16),
            pltpu.VMEM((n, r, w), bf16),
            pltpu.VMEM((clusters, leaf, w), bf16),
            pltpu.VMEM((clusters, 1, w), f32),
            pltpu.VMEM((16, r, w), bf16),
            pltpu.VMEM((4, 2, r // 2, w), bf16),
            pltpu.VMEM((4, 2, r, w), bf16),
            pltpu.VMEM((2, r // 2, w), bf16),
            pltpu.VMEM((2, r, w), bf16),
            pltpu.VMEM((2, clusters, leaf // 4, w), bf16),
            pltpu.VMEM((2, 2, leaf // 4, w), bf16),
            pltpu.VMEM((2, clusters, leaf // 4, w), bf16),
            pltpu.VMEM((4, 1, w), f32),
            dma((52,)),
            dma((48,)),
            dma((2, 32)),
            dma((2, 32)),
        ],
        compiler_params=pltpu.CompilerParams(
            collective_id=1, has_side_effects=True, vmem_limit_bytes=67043328
        ),
    )(labels, match, info, lse, scores, rec)


def body(queries, labels, matcher, cluster_ids, positives):
    q_dev, width = queries.shape
    cl_dev = labels.shape[0]
    n_label = lax.axis_size("label")
    first = lax.axis_index("label") * cl_dev
    match = lax.dynamic_slice_in_dim(matcher, first, cl_dev, 0).reshape(cl_dev, 1, width)
    ids = cluster_ids.reshape(n_label, q_dev, K).transpose(0, 2, 1)
    pos = positives.reshape(n_label, 1, q_dev)
    scores, received, info, lse, losses = forward(queries, labels, match, ids, pos)
    query_grads, label_grads, rows = backward(labels, match, info, lse, scores, received)
    matcher_grads = rows.transpose(1, 0, 2, 3).reshape(matcher.shape)
    return (losses.reshape(q_dev), query_grads, label_grads, matcher_grads)


def solution(mesh):
    return jax.shard_map(
        body,
        mesh=mesh,
        in_specs=(P(("dp", "label"), None), P("label", None, None), P(), P("dp", None), P("dp")),
        out_specs=(P(("dp", "label")), P(("dp", "label"), None), P("label", "dp", None), P()),
        check_vma=False,
    )
```

```python
import jax
import jax.numpy as jnp
from jax import lax
from jax.experimental import pallas as pl
from jax.experimental.pallas import tpu as pltpu
from jax.sharding import PartitionSpec as P

LEAF = 512
K = 16
BIG = 1e30

MESH = pl.DeviceIdType.MESH

def place():
    me = lax.axis_index("label")
    core = lax.rem(me, 2)
    x = lax.rem(me // 2, 4)
    y = me // 8
    a = x * (1 - core) + y * core
    b = y * (1 - core) + x * core
    return me, core, a, b

def index_of(core, a, b):
    x = a * (1 - core) + b * core
    y = b * (1 - core) + a * core
    return (y * 4 + x) * 2 + core

OFF = (0, 3, 1, 2)

class Links:
    def __init__(self, send, recv):
        self.me, self.core, self.a, self.b = place()
        self.send, self.recv, self.sent = send, recv, []
        c, a, b = self.core, self.a, self.b
        self.partner = self.me + 1 - 2 * c
        self.dev = {
            "a-": index_of(c, lax.rem(a + 3, 4), b),
            "a+": index_of(c, lax.rem(a + 1, 4), b),
            "b-": index_of(c, a, lax.rem(b + 3, 4)),
            "b+": index_of(c, a, lax.rem(b + 1, 4)),
            "p": self.partner,
        }
    def block(self, i, j):
        return index_of(self.core, lax.rem(self.a + OFF[i], 4), lax.rem(self.b + OFF[j], 4))
    def partner_block(self, i, j):
        return index_of(1 - self.core, lax.rem(self.b + OFF[i], 4), lax.rem(self.a + OFF[j], 4))
    def meet(self, peers=None):
        barrier = pltpu.get_barrier_semaphore()
        peers = list(self.dev.values()) if peers is None else peers
        for d in peers:
            pl.semaphore_signal(barrier, inc=1, device_id={"label": d}, device_id_type=MESH)
        pl.semaphore_wait(barrier, len(peers))
    def copy(self, src, dst, slot, to):
        n = len(self.sent)
        c = pltpu.make_async_remote_copy(src_ref=src, dst_ref=dst, send_sem=self.send.at[n],
            recv_sem=self.recv.at[slot], device_id={"label": self.dev[to]}, device_id_type=MESH)
        c.start()
        self.sent.append(c)
    def wait(self, dst, slot):
        pltpu.make_async_remote_copy(src_ref=dst, dst_ref=dst, send_sem=self.send.at[0],
            recv_sem=self.recv.at[slot], device_id={"label": self.partner}, device_id_type=MESH).wait_recv()
    def drain(self):
        for c in self.sent:
            c.wait_send()


SLOTS = 48
TURNS = (
    ((0, 0), (1, 0), (2, 0), (0, 1), (0, 2)),
    ((3, 0), (0, 3), (1, 1), (1, 2)),
    ((2, 1), (2, 2), (1, 3), (3, 1), (3, 2)),
    ((2, 3), (3, 3)),
)


def slot_tables(ids, pos):
    f32 = jnp.float32
    n = ids.shape[1]
    rows = lax.broadcasted_iota(jnp.int32, ids.shape, 0)
    pos_cluster = jnp.sum(
        jnp.where(rows == (pos >> 9), ids, 0).astype(f32), axis=0, keepdims=True
    )
    line = lax.broadcasted_iota(jnp.int32, (8, n), 0)
    named = jnp.zeros((8, n), f32)
    for c in range(4):
        hit = jnp.sum((ids == c).astype(f32), axis=0, keepdims=True)
        named = jnp.where(line == c, hit, named)
    earlier = (
        lax.broadcasted_iota(jnp.int32, (n, n), 0) < lax.broadcasted_iota(jnp.int32, (n, n), 1)
    ).astype(f32)
    rank = jnp.dot(
        named.astype(jnp.bfloat16), earlier.astype(jnp.bfloat16), preferred_element_type=f32
    )
    code = jnp.where(named > 0.5, rank, -1.0)
    target = ((pos & (LEAF - 1)) + 1).astype(f32)
    targets = jnp.where(pos_cluster == (line - 4).astype(f32), target, 0.0)
    return jnp.where(line < 4, code, targets)


def picks(info, c):
    r = lax.broadcasted_iota(jnp.int32, (SLOTS, info.shape[1]), 0).astype(jnp.float32)
    return info[c : c + 1] == r


def target_column(info, pick, c):
    return jnp.sum(jnp.where(pick, info[4 + c : 5 + c], 0.0), axis=1, keepdims=True) - 1.0


def forward_kernel(q_ref, labels, match, ids_ref, pos_ref, scores_out, rec_out, info, lse, losses,
                   g, scores, rec, st, sr, send, recv, st_send, st_recv, lse_send, lse_recv, out_sem):
    f32 = jnp.float32
    L = Links(send, recv)
    peers = [(k, L.block(i, j)) for k, (i, j) in enumerate([(i, j) for i in range(4) for j in range(4)])]
    peers = [d for k, d in peers if k > 0]
    peers += [L.partner_block(i, j) for i in range(4) for j in range(4)]
    L.meet(peers)
    half = q_ref.shape[0] // 2
    first = L.me * 4
    lo = lambda k: g.at[k, pl.ds(0, half)]
    hi = lambda k: g.at[k, pl.ds(half, half)]
    own = L.block(0, 0)
    for to, slot in (("a+", 0), ("a-", 1), ("b+", 4), ("b-", 5), ("p", 20)):
        L.copy(q_ref, g.at[own], slot, to)
    g[own] = q_ref[...]

    def tables(s, carry):
        info[s] = slot_tables(ids_ref[s] - first, pos_ref[s])
        return carry

    lax.fori_loop(0, 32, tables, 0)

    def side_a(i):
        k = L.block(i, 0)
        L.wait(g.at[k], i - 1)
        if i == 1:
            L.copy(lo(k), lo(k), 2, "a+")
        else:
            L.copy(hi(k), hi(k), 3, "a-")
        L.copy(g.at[k], g.at[k], 4 + 4 * i, "b+")
        L.copy(g.at[k], g.at[k], 5 + 4 * i, "b-")
        L.copy(g.at[k], g.at[k], 20 + 4 * i, "p")

    def far_a():
        k = L.block(3, 0)
        L.wait(lo(k), 2)
        L.wait(hi(k), 3)
        L.copy(g.at[k], g.at[k], 16, "b+")
        L.copy(g.at[k], g.at[k], 17, "b-")
        L.copy(g.at[k], g.at[k], 32, "p")

    def side_b(i):
        k = L.block(i, 1)
        L.wait(g.at[k], 4 + 4 * i)
        L.copy(lo(k), lo(k), 6 + 4 * i, "b+")
        L.copy(g.at[k], g.at[k], 21 + 4 * i, "p")
        k = L.block(i, 2)
        L.wait(g.at[k], 5 + 4 * i)
        L.copy(hi(k), hi(k), 7 + 4 * i, "b-")
        L.copy(g.at[k], g.at[k], 22 + 4 * i, "p")

    def far_b(i):
        k = L.block(i, 3)
        L.wait(lo(k), 6 + 4 * i)
        L.wait(hi(k), 7 + 4 * i)
        L.copy(g.at[k], g.at[k], 23 + 4 * i, "p")

    def work(turn, middle):
        members = TURNS[turn]
        size = len(members)
        base = 2 * sum(len(t) for t in TURNS[:turn])
        for i, j in members:
            L.wait(g.at[L.partner_block(i, j)], 20 + 4 * i + j)
        code_a = sum(OFF[i] << (2 * n) for n, (i, j) in enumerate(members))
        code_b = sum(OFF[j] << (2 * n) for n, (i, j) in enumerate(members))

        def block_of(n):
            other, m = n // size, lax.rem(n, size)
            core = L.core + other - 2 * L.core * other
            da = lax.rem(lax.shift_right_logical(jnp.int32(code_a), 2 * m), 4)
            db = lax.rem(lax.shift_right_logical(jnp.int32(code_b), 2 * m), 4)
            a = lax.rem(L.a * (1 - other) + L.b * other + da, 4)
            b = lax.rem(L.b * (1 - other) + L.a * other + db, 4)
            return index_of(core, a, b)

        blocks = [L.block(i, j) for i, j in members] + [L.partner_block(i, j) for i, j in members]

        def pick(n, carry):
            s = block_of(n)
            table = info[s]
            one = jnp.concatenate([picks(table, c).astype(f32) for c in range(4)], axis=0)
            rows = jnp.dot(one.astype(jnp.bfloat16), g[s], preferred_element_type=f32)
            rec[s] = rows.astype(jnp.bfloat16).reshape(4, SLOTS, rows.shape[1])
            return carry

        lax.fori_loop(0, 2 * size, pick, 0)
        middle()

        def score(c, carry):
            rows = jnp.concatenate([rec[k, c] for k in blocks], axis=0)
            out = lax.dot_general(rows, labels[c], (((1,), (1,)), ((), ())), preferred_element_type=f32)
            bias = jnp.sum(rows.astype(f32) * match[c].astype(f32), axis=1, keepdims=True)
            out = out + bias
            for n, k in enumerate(blocks):
                scores[k, c] = out[n * SLOTS : (n + 1) * SLOTS]
            return carry

        lax.fori_loop(0, 4, score, 0)

        def stat(n, carry):
            s = block_of(n)
            table = info[s]
            leaf = lax.broadcasted_iota(jnp.int32, (SLOTS, LEAF), 1).astype(f32)
            parts = []
            for c in range(4):
                one = picks(table, c)
                val = scores[s, c]
                top = jnp.max(val, axis=1, keepdims=True)
                total = jnp.sum(jnp.exp(val - top), axis=1, keepdims=True)
                picked = jnp.sum(
                    jnp.where(leaf == target_column(table, one, c), val, 0.0), axis=1, keepdims=True
                )
                parts.append((one, top, total, picked))
            best = jnp.full((1, table.shape[1]), -BIG, f32)
            for one, top, total, picked in parts:
                best = jnp.maximum(best, jnp.max(jnp.where(one, top, -BIG), axis=0, keepdims=True))
            spread = jnp.zeros_like(best)
            chosen = jnp.zeros_like(best)
            for one, top, total, picked in parts:
                spread += jnp.sum(
                    jnp.where(one, total * jnp.exp(jnp.where(one, top - best, 0.0)), 0.0), axis=0, keepdims=True
                )
                chosen += jnp.sum(jnp.where(one, picked, 0.0), axis=0, keepdims=True)
            st[s] = jnp.concatenate([best, spread, chosen], axis=1)
            return carry

        lax.fori_loop(0, 2 * size, stat, 0)
        for m, k in enumerate(blocks):
            n = base + m
            pltpu.make_async_copy(scores.at[k], scores_out.at[k], out_sem.at[2 * n]).start()
            pltpu.make_async_copy(rec.at[k], rec_out.at[k], out_sem.at[2 * n + 1]).start()
            if n == 0:
                continue
            pltpu.make_async_remote_copy(
                src_ref=st.at[k], dst_ref=sr.at[L.me], send_sem=st_send.at[k], recv_sem=st_recv.at[L.me],
                device_id={"label": k}, device_id_type=MESH,
            ).start()
        return blocks

    side_a(1)
    side_a(2)
    side_b(0)
    order = work(0, far_a)
    far_b(0)
    side_b(1)
    order += work(1, lambda: side_b(2))
    far_b(1)
    side_b(3)
    order += work(2, lambda: far_b(2))
    far_b(3)
    order += work(3, lambda: None)
    sr[own] = st[own]

    def stat_copy(k, arrive):
        return pltpu.make_async_remote_copy(
            src_ref=st.at[k], dst_ref=sr.at[k], send_sem=st_send.at[k], recv_sem=st_recv.at[k],
            device_id={"label": k}, device_id_type=MESH,
        )

    for k in peers:
        stat_copy(k, True).wait_recv()
    q_dev = q_ref.shape[0]
    tops = sr[:, :, 0:q_dev]
    best = jnp.max(tops, axis=0)
    spread = jnp.sum(sr[:, :, q_dev : 2 * q_dev] * jnp.exp(tops - best[None]), axis=0)
    chosen = jnp.sum(sr[:, :, 2 * q_dev : 3 * q_dev], axis=0)
    value = best + jnp.log(spread)
    losses[...] = value - chosen
    lse[own] = value

    def lse_copy(dev, row):
        return pltpu.make_async_remote_copy(
            src_ref=lse.at[row], dst_ref=lse.at[row], send_sem=lse_send.at[dev], recv_sem=lse_recv.at[row],
            device_id={"label": dev}, device_id_type=MESH,
        )

    for k in peers:
        lse_copy(k, own).start()
    for k in peers:
        lse_copy(k, k).wait_recv()
    for k in peers:
        stat_copy(k, False).wait_send()
        lse_copy(k, own).wait_send()
    for n, k in enumerate(order):
        pltpu.make_async_copy(scores.at[k], scores_out.at[k], out_sem.at[2 * n]).wait()
        pltpu.make_async_copy(rec.at[k], rec_out.at[k], out_sem.at[2 * n + 1]).wait()
    L.drain()


def forward(q, labels, match, ids, pos):
    q_dev, width = q.shape
    vmem = pl.BlockSpec(memory_space=pltpu.VMEM)
    hbm = pl.BlockSpec(memory_space=pl.ANY)
    shape = jax.ShapeDtypeStruct
    f32, bf16, dma = jnp.float32, jnp.bfloat16, pltpu.SemaphoreType.DMA
    return pl.pallas_call(
        forward_kernel,
        out_shape=(
            shape((32, 4, SLOTS, LEAF), f32),
            shape((32, 4, SLOTS, width), bf16),
            shape((32, 8, q_dev), f32),
            shape((32, 1, q_dev), f32),
            shape((1, q_dev), f32),
        ),
        in_specs=[vmem] * 5,
        out_specs=(hbm, hbm, vmem, vmem, vmem),
        scratch_shapes=[
            pltpu.VMEM((32, q_dev, width), bf16),
            pltpu.VMEM((32, 4, SLOTS, LEAF), f32),
            pltpu.VMEM((32, 4, SLOTS, width), bf16),
            pltpu.VMEM((32, 1, 3 * q_dev), f32),
            pltpu.VMEM((32, 1, 3 * q_dev), f32),
            dma((36,)), dma((36,)), dma((32,)), dma((32,)), dma((32,)), dma((32,)), dma((64,)),
        ],
        compiler_params=pltpu.CompilerParams(
            collective_id=0, has_side_effects=True, vmem_limit_bytes=60 * 1024 * 1024
        ),
    )(q, labels, match, ids, pos)


class Column:
    def __init__(self, links):
        self.z = lax.axis_index("dp")
        self.links = links

    def copy(self, src, dst, slot, off):
        L = self.links
        n = len(L.sent)
        c = pltpu.make_async_remote_copy(
            src_ref=src, dst_ref=dst, send_sem=L.send.at[n], recv_sem=L.recv.at[slot],
            device_id={"dp": lax.rem(self.z + off, 4)}, device_id_type=MESH,
        )
        c.start()
        L.sent.append(c)


BACK_TURNS = (
    ((3, 3), (3, 1), (3, 2), (1, 3)),
    ((2, 3), (3, 0), (1, 1), (1, 2)),
    ((2, 1), (2, 2), (0, 3), (1, 0)),
    ((2, 0), (0, 1), (0, 2), (0, 0)),
)


def backward_kernel(labels, match, info, lse, scores_hbm, rec_hbm, out, label_out, matcher_out,
                    mout, stage, rec, delta, coef, grads, p, lp, ls, pr, bh, bf, ah, af, zh, zf, mz,
                    send, recv, m_recv, in_sem):
    L = Links(send, recv)
    Z = Column(L)
    z = Z.z
    f32, bf16 = jnp.float32, jnp.bfloat16
    turns = [
        [L.block(i, j) for i, j in t] + [L.partner_block(i, j) for i, j in t] for t in BACK_TURNS
    ]

    def load_scores(t):
        return [
            pltpu.make_async_copy(scores_hbm.at[k], stage.at[t % 2, m], in_sem.at[0, 8 * t + m])
            for m, k in enumerate(turns[t])
        ]

    def load_rows(t):
        return [
            pltpu.make_async_copy(rec_hbm.at[k], rec.at[k], in_sem.at[1, 8 * t + m])
            for m, k in enumerate(turns[t])
        ]

    for t in range(2):
        for c in load_scores(t) + load_rows(t):
            c.start()
    for t in range(2, 4):
        for c in load_rows(t):
            c.start()
    peers = [L.block(i, j) for i in range(4) for j in range(4)][1:]
    peers += [L.partner_block(i, j) for i in range(4) for j in range(4)]
    barrier = pltpu.get_barrier_semaphore()
    for d in peers:
        pl.semaphore_signal(barrier, inc=1, device_id={"label": d}, device_id_type=MESH)
    for off in (1, 2, 3):
        pl.semaphore_signal(barrier, inc=1, device_id={"dp": lax.rem(z + off, 4)}, device_id_type=MESH)
    ls[...] = jnp.zeros_like(ls)

    def block_of(t, n):
        code_a = sum(OFF[i] << (2 * m) for m, (i, j) in enumerate(BACK_TURNS[t]))
        code_b = sum(OFF[j] << (2 * m) for m, (i, j) in enumerate(BACK_TURNS[t]))
        other, m = n // 4, lax.rem(n, 4)
        core = L.core + other - 2 * L.core * other
        da = lax.rem(lax.shift_right_logical(jnp.int32(code_a), 2 * m), 4)
        db = lax.rem(lax.shift_right_logical(jnp.int32(code_b), 2 * m), 4)
        a = lax.rem(L.a * (1 - other) + L.b * other + da, 4)
        b = lax.rem(L.b * (1 - other) + L.a * other + db, 4)
        return index_of(core, a, b)

    def part(t):
        for c in load_scores(t) + load_rows(t):
            c.wait()

        def step(n, carry):
            k = block_of(t, n)
            table = info[k]
            leaf = lax.broadcasted_iota(jnp.int32, (SLOTS, LEAF), 1).astype(f32)
            log_sum = lse[k]
            for c in range(4):
                one = picks(table, c)
                used = jnp.sum(jnp.where(one, 1.0, 0.0), axis=1, keepdims=True) > 0.5
                norm = jnp.sum(jnp.where(one, log_sum, 0.0), axis=1, keepdims=True)
                norm = jnp.where(used, norm, BIG)
                hit = leaf == target_column(table, one, c)
                value = jnp.exp(stage[t % 2, n, c] - norm) - hit.astype(f32)
                total = jnp.sum(value, axis=1, keepdims=True).astype(bf16)
                delta[k, c] = value.astype(bf16)
                coef[k, c] = jnp.broadcast_to(total.astype(f32), (SLOTS, 128)).astype(bf16)
                ls[c] += jnp.sum(total.astype(f32) * rec[k, c].astype(f32), axis=0, keepdims=True)
            return carry

        lax.fori_loop(0, 8, step, 0)
        if t < 2:
            for c in load_scores(t + 2):
                c.start()

    def slots(t):
        def slot(c, carry):
            rows = jnp.concatenate([delta[k, c] for k in turns[t]], axis=0)
            scale = jnp.concatenate([coef[k, c] for k in turns[t]], axis=0)[:, 0:1].astype(f32)
            val = jnp.dot(rows, labels[c], preferred_element_type=f32)
            val = (val + scale * match[c].astype(f32)).astype(bf16)
            for n in range(8):
                grads[n, pl.ds(pl.multiple_of(c * SLOTS, 16), SLOTS)] = val[n * SLOTS : (n + 1) * SLOTS]
            return carry

        lax.fori_loop(0, 4, slot, 0)

        def back(n, carry):
            k = block_of(t, n)
            table = info[k]
            one = jnp.concatenate([picks(table, c).astype(f32) for c in range(4)], axis=0).astype(bf16)
            val = lax.dot_general(one, grads[n], (((0,), (0,)), ((), ())), preferred_element_type=f32)
            p[k] = val.astype(bf16)
            return carry

        lax.fori_loop(0, 8, back, 0)
        for i, j in BACK_TURNS[t]:
            L.copy(p.at[L.partner_block(i, j)], pr.at[4 * i + j], 4 * i + j, "p")

    def label_parts(low):
        def one_part(c, carry):
            left = jnp.concatenate([delta[k, c] for k in range(32)], axis=0)
            right = jnp.concatenate([rec[k, c] for k in range(32)], axis=0)
            val = lax.dot_general(left, right, (((0,), (0,)), ((), ())), preferred_element_type=f32)
            lp[c] = val.astype(bf16)
            return carry

        lax.fori_loop(low, low + 2, one_part, 0)

    half = p.shape[1] // 2
    rows_z = label_out.shape[1]

    def rows(off):
        return pl.ds(pl.multiple_of(lax.rem(z + off, 4) * rows_z, rows_z), rows_z)

    PAIRS = pl.ds(0, 2), pl.ds(2, 2)
    LO, HI = pl.ds(0, half), pl.ds(half, half)

    def both(i, j):
        L.wait(pr.at[4 * i + j], 4 * i + j)
        return lambda s: p[L.block(i, j), s].astype(f32) + pr[4 * i + j, s].astype(f32)

    def far(i):
        s = both(i, 3)
        t = p.at[L.block(i, 3)]
        t[...] = s(slice(None)).astype(t.dtype)
        L.copy(t.at[LO], bh.at[i, 0], 16 + 4 * i, "b+")
        L.copy(t.at[HI], bh.at[i, 1], 17 + 4 * i, "b-")

    def near(i):
        s = both(i, 2)
        t = p.at[L.block(i, 2)]
        L.wait(bh.at[i, 0], 16 + 4 * i)
        t[LO] = (s(LO) + bh[i, 0].astype(f32)).astype(t.dtype)
        t[HI] = s(HI).astype(t.dtype)
        L.copy(t, bf.at[i, 0], 18 + 4 * i, "b+")
        s = both(i, 1)
        t = p.at[L.block(i, 1)]
        L.wait(bh.at[i, 1], 17 + 4 * i)
        t[HI] = (s(HI) + bh[i, 1].astype(f32)).astype(t.dtype)
        t[LO] = s(LO).astype(t.dtype)
        L.copy(t, bf.at[i, 1], 19 + 4 * i, "b-")

    def column(i):
        s = both(i, 0)
        L.wait(bf.at[i, 0], 18 + 4 * i)
        L.wait(bf.at[i, 1], 19 + 4 * i)
        return lambda r: s(r) + bf[i, 0, r].astype(f32) + bf[i, 1, r].astype(f32)

    def row_copy(dev, row):
        return pltpu.make_async_remote_copy(
            src_ref=mout.at[z, row], dst_ref=mout.at[z, row], send_sem=m_recv.at[1, dev], recv_sem=m_recv.at[0, row],
            device_id={"label": dev}, device_id_type=MESH,
        )

    def opposite():
        s = column(3)
        u = p.at[L.block(3, 0)]
        u[...] = s(slice(None)).astype(u.dtype)
        L.copy(u.at[LO], ah.at[0], 32, "a+")
        L.copy(u.at[HI], ah.at[1], 33, "a-")

    def beside_minus():
        s = column(1)
        u = p.at[L.block(1, 0)]
        L.wait(ah.at[1], 33)
        u[HI] = (s(HI) + ah[1].astype(f32)).astype(u.dtype)
        u[LO] = s(LO).astype(u.dtype)
        L.copy(u, af.at[1], 35, "a-")

    def beside_plus():
        s = column(2)
        u = p.at[L.block(2, 0)]
        L.wait(ah.at[0], 32)
        u[LO] = (s(LO) + ah[0].astype(f32)).astype(u.dtype)
        u[HI] = s(HI).astype(u.dtype)
        L.copy(u, af.at[0], 34, "a+")

    part(0)
    pl.semaphore_wait(barrier, 34)
    slots(0)
    part(1)
    far(3)
    far(1)
    part(2)
    part(3)
    mz[z] = ls[z]
    for off in (1, 2, 3):
        Z.copy(ls.at[lax.rem(z + off, 4)], mz.at[z], 41 + off, off)
    label_parts(0)
    Z.copy(lp.at[PAIRS[0], rows(2)], zh.at[0], 36, 1)
    near(3)
    label_parts(2)
    Z.copy(lp.at[PAIRS[1], rows(2)], zh.at[1], 37, 3)
    slots(1)
    far(2)
    near(1)
    for off in (1, 2, 3):
        L.wait(mz.at[lax.rem(z + 4 - off, 4)], 41 + off)
    mout[z, L.me] = mz[0] + mz[1] + mz[2] + mz[3]
    for k in peers:
        row_copy(k, L.me).start()
    slots(2)
    opposite()
    far(0)
    near(2)
    L.wait(zh.at[0], 36)
    lp[PAIRS[0], rows(1)] = (lp[PAIRS[0], rows(1)].astype(f32) + zh[0].astype(f32)).astype(bf16)
    Z.copy(lp.at[:, rows(1)], zf.at[0], 38, 1)
    L.wait(zh.at[1], 37)
    lp[PAIRS[1], rows(3)] = (lp[PAIRS[1], rows(3)].astype(f32) + zh[1].astype(f32)).astype(bf16)
    Z.copy(lp.at[:, rows(3)], zf.at[1], 39, 3)
    beside_minus()
    slots(3)
    near(0)
    beside_plus()
    for k in peers:
        row_copy(k, k).wait_recv()
    for off in (1, 2, 3):
        Z.copy(mout.at[z], mout.at[z], 44 + off, off)
    L.wait(zf.at[0], 38)
    L.wait(zf.at[1], 39)
    label_out[...] = lp[:, rows(0)].astype(f32) + zf[0].astype(f32) + zf[1].astype(f32)
    s = column(0)
    L.wait(af.at[0], 34)
    L.wait(af.at[1], 35)
    out[...] = s(slice(None)) + af[0].astype(f32) + af[1].astype(f32)
    for off in (1, 2, 3):
        L.wait(mout.at[lax.rem(z + 4 - off, 4)], 44 + off)
    for k in range(32):
        for c in range(4):
            matcher_out[4 * k + c : 4 * k + c + 1] = mout[c, k]
    for k in peers:
        row_copy(k, L.me).wait_send()
    L.drain()


def backward(labels, match, info, lse, scores, rec):
    n, _, r = info.shape
    clusters, leaf, w = labels.shape
    f32, bf16, dma = jnp.float32, jnp.bfloat16, pltpu.SemaphoreType.DMA
    vmem = pl.BlockSpec(memory_space=pltpu.VMEM)
    hbm = pl.BlockSpec(memory_space=pl.ANY)
    shape = jax.ShapeDtypeStruct
    return pl.pallas_call(
        backward_kernel,
        out_shape=(shape((r, w), f32), shape((clusters, leaf // 4, w), f32), shape((4 * n, w), f32)),
        in_specs=[vmem] * 4 + [hbm] * 2,
        out_specs=(vmem,) * 3,
        scratch_shapes=[
            pltpu.VMEM((4, n, 1, w), f32),
            pltpu.VMEM((2, 8, 4, SLOTS, leaf), f32),
            pltpu.VMEM((n, 4, SLOTS, w), bf16),
            pltpu.VMEM((n, 4, SLOTS, leaf), bf16),
            pltpu.VMEM((n, 4, SLOTS, 128), bf16),
            pltpu.VMEM((8, 4 * SLOTS, w), bf16),
            pltpu.VMEM((n, r, w), bf16),
            pltpu.VMEM((clusters, leaf, w), bf16),
            pltpu.VMEM((clusters, 1, w), f32),
            pltpu.VMEM((16, r, w), bf16),
            pltpu.VMEM((4, 2, r // 2, w), bf16),
            pltpu.VMEM((4, 2, r, w), bf16),
            pltpu.VMEM((2, r // 2, w), bf16),
            pltpu.VMEM((2, r, w), bf16),
            pltpu.VMEM((2, 2, leaf // 4, w), bf16),
            pltpu.VMEM((2, clusters, leaf // 4, w), bf16),
            pltpu.VMEM((4, 1, w), f32),
            dma((52,)),
            dma((48,)),
            dma((2, 32)),
            dma((2, 32)),
        ],
        compiler_params=pltpu.CompilerParams(
            collective_id=1, has_side_effects=True, vmem_limit_bytes=67043328
        ),
    )(labels, match, info, lse, scores, rec)


def body(queries, labels, matcher, cluster_ids, positives):
    q_dev, width = queries.shape
    cl_dev = labels.shape[0]
    n_label = lax.axis_size("label")
    first = lax.axis_index("label") * cl_dev
    match = lax.dynamic_slice_in_dim(matcher, first, cl_dev, 0).reshape(cl_dev, 1, width)
    ids = cluster_ids.reshape(n_label, q_dev, K).transpose(0, 2, 1)
    pos = positives.reshape(n_label, 1, q_dev)
    scores, received, info, lse, losses = forward(queries, labels, match, ids, pos)
    query_grads, label_grads, matcher_grads = backward(
        labels, match, info, lse, scores, received
    )
    return (losses.reshape(q_dev), query_grads, label_grads, matcher_grads)


def solution(mesh):
    return jax.shard_map(
        body,
        mesh=mesh,
        in_specs=(P(("dp", "label"), None), P("label", None, None), P(), P("dp", None), P("dp")),
        out_specs=(P(("dp", "label")), P(("dp", "label"), None), P("label", "dp", None), P()),
        check_vma=False,
    )
```

```python
import jax
import jax.numpy as jnp
from jax import lax
from jax.experimental import pallas as pl
from jax.experimental.pallas import tpu as pltpu
from jax.sharding import PartitionSpec as P

LEAF = 512
K = 16
BIG = 1e30

MESH = pl.DeviceIdType.MESH

def place():
    me = lax.axis_index("label")
    core = lax.rem(me, 2)
    x = lax.rem(me // 2, 4)
    y = me // 8
    a = x * (1 - core) + y * core
    b = y * (1 - core) + x * core
    return me, core, a, b

def index_of(core, a, b):
    x = a * (1 - core) + b * core
    y = b * (1 - core) + a * core
    return (y * 4 + x) * 2 + core

OFF = (0, 3, 1, 2)

def in_pairs(count, step):
    def two(n, carry):
        step(2 * n, 0)
        step(2 * n + 1, 0)
        return carry

    lax.fori_loop(0, count // 2, two, 0)


class Links:
    def __init__(self, send, recv):
        self.me, self.core, self.a, self.b = place()
        self.send, self.recv, self.sent = send, recv, []
        c, a, b = self.core, self.a, self.b
        self.partner = self.me + 1 - 2 * c
        self.dev = {
            "a-": index_of(c, lax.rem(a + 3, 4), b),
            "a+": index_of(c, lax.rem(a + 1, 4), b),
            "b-": index_of(c, a, lax.rem(b + 3, 4)),
            "b+": index_of(c, a, lax.rem(b + 1, 4)),
            "p": self.partner,
        }
    def block(self, i, j):
        return index_of(self.core, lax.rem(self.a + OFF[i], 4), lax.rem(self.b + OFF[j], 4))
    def partner_block(self, i, j):
        return index_of(1 - self.core, lax.rem(self.b + OFF[i], 4), lax.rem(self.a + OFF[j], 4))
    def meet(self, peers=None):
        barrier = pltpu.get_barrier_semaphore()
        peers = list(self.dev.values()) if peers is None else peers
        for d in peers:
            pl.semaphore_signal(barrier, inc=1, device_id={"label": d}, device_id_type=MESH)
        pl.semaphore_wait(barrier, len(peers))
    def copy(self, src, dst, slot, to):
        n = len(self.sent)
        c = pltpu.make_async_remote_copy(src_ref=src, dst_ref=dst, send_sem=self.send.at[n],
            recv_sem=self.recv.at[slot], device_id={"label": self.dev[to]}, device_id_type=MESH)
        c.start()
        self.sent.append(c)
    def wait(self, dst, slot):
        pltpu.make_async_remote_copy(src_ref=dst, dst_ref=dst, send_sem=self.send.at[0],
            recv_sem=self.recv.at[slot], device_id={"label": self.partner}, device_id_type=MESH).wait_recv()
    def drain(self):
        for c in self.sent:
            c.wait_send()


SLOTS = 48
TURNS = (
    ((0, 0), (1, 0), (2, 0), (0, 1), (0, 2)),
    ((3, 0), (0, 3), (1, 1), (1, 2)),
    ((2, 1), (2, 2), (1, 3), (3, 1), (3, 2)),
    ((2, 3), (3, 3)),
)


def slot_tables(ids, pos):
    f32 = jnp.float32
    n = ids.shape[1]
    rows = lax.broadcasted_iota(jnp.int32, ids.shape, 0)
    pos_cluster = jnp.sum(
        jnp.where(rows == (pos >> 9), ids, 0).astype(f32), axis=0, keepdims=True
    )
    line = lax.broadcasted_iota(jnp.int32, (8, n), 0)
    named = jnp.zeros((8, n), f32)
    for c in range(4):
        hit = jnp.sum((ids == c).astype(f32), axis=0, keepdims=True)
        named = jnp.where(line == c, hit, named)
    earlier = (
        lax.broadcasted_iota(jnp.int32, (n, n), 0) < lax.broadcasted_iota(jnp.int32, (n, n), 1)
    ).astype(f32)
    rank = jnp.dot(
        named.astype(jnp.bfloat16), earlier.astype(jnp.bfloat16), preferred_element_type=f32
    )
    code = jnp.where(named > 0.5, rank, -1.0)
    target = ((pos & (LEAF - 1)) + 1).astype(f32)
    targets = jnp.where(pos_cluster == (line - 4).astype(f32), target, 0.0)
    return jnp.where(line < 4, code, targets)


def picks(info, c):
    r = lax.broadcasted_iota(jnp.int32, (SLOTS, info.shape[1]), 0).astype(jnp.float32)
    return info[c : c + 1] == r


def target_column(info, pick, c):
    return jnp.sum(jnp.where(pick, info[4 + c : 5 + c], 0.0), axis=1, keepdims=True) - 1.0


def forward_kernel(q_ref, labels, match, ids_ref, pos_ref, scores_out, rec_out, info, lse, losses,
                   g, scores, rec, st, sr, send, recv, st_send, st_recv, lse_send, lse_recv, out_sem):
    f32 = jnp.float32
    L = Links(send, recv)
    peers = [(k, L.block(i, j)) for k, (i, j) in enumerate([(i, j) for i in range(4) for j in range(4)])]
    peers = [d for k, d in peers if k > 0]
    peers += [L.partner_block(i, j) for i in range(4) for j in range(4)]
    L.meet(peers)
    half = q_ref.shape[0] // 2
    first = L.me * 4
    lo = lambda k: g.at[k, pl.ds(0, half)]
    hi = lambda k: g.at[k, pl.ds(half, half)]
    own = L.block(0, 0)
    for to, slot in (("a+", 0), ("a-", 1), ("b+", 4), ("b-", 5), ("p", 20)):
        L.copy(q_ref, g.at[own], slot, to)
    g[own] = q_ref[...]

    def tables(s, carry):
        info[s] = slot_tables(ids_ref[s] - first, pos_ref[s])
        return carry

    in_pairs(32, tables)

    def side_a(i):
        k = L.block(i, 0)
        L.wait(g.at[k], i - 1)
        if i == 1:
            L.copy(lo(k), lo(k), 2, "a+")
        else:
            L.copy(hi(k), hi(k), 3, "a-")
        L.copy(g.at[k], g.at[k], 4 + 4 * i, "b+")
        L.copy(g.at[k], g.at[k], 5 + 4 * i, "b-")
        L.copy(g.at[k], g.at[k], 20 + 4 * i, "p")

    def far_a():
        k = L.block(3, 0)
        L.wait(lo(k), 2)
        L.wait(hi(k), 3)
        L.copy(g.at[k], g.at[k], 16, "b+")
        L.copy(g.at[k], g.at[k], 17, "b-")
        L.copy(g.at[k], g.at[k], 32, "p")

    def side_b(i):
        k = L.block(i, 1)
        L.wait(g.at[k], 4 + 4 * i)
        L.copy(lo(k), lo(k), 6 + 4 * i, "b+")
        L.copy(g.at[k], g.at[k], 21 + 4 * i, "p")
        k = L.block(i, 2)
        L.wait(g.at[k], 5 + 4 * i)
        L.copy(hi(k), hi(k), 7 + 4 * i, "b-")
        L.copy(g.at[k], g.at[k], 22 + 4 * i, "p")

    def far_b(i):
        k = L.block(i, 3)
        L.wait(lo(k), 6 + 4 * i)
        L.wait(hi(k), 7 + 4 * i)
        L.copy(g.at[k], g.at[k], 23 + 4 * i, "p")

    def work(turn, middle):
        members = TURNS[turn]
        size = len(members)
        base = 2 * sum(len(t) for t in TURNS[:turn])
        for i, j in members:
            L.wait(g.at[L.partner_block(i, j)], 20 + 4 * i + j)
        code_a = sum(OFF[i] << (2 * n) for n, (i, j) in enumerate(members))
        code_b = sum(OFF[j] << (2 * n) for n, (i, j) in enumerate(members))

        def block_of(n):
            other, m = n // size, lax.rem(n, size)
            core = L.core + other - 2 * L.core * other
            da = lax.rem(lax.shift_right_logical(jnp.int32(code_a), 2 * m), 4)
            db = lax.rem(lax.shift_right_logical(jnp.int32(code_b), 2 * m), 4)
            a = lax.rem(L.a * (1 - other) + L.b * other + da, 4)
            b = lax.rem(L.b * (1 - other) + L.a * other + db, 4)
            return index_of(core, a, b)

        blocks = [L.block(i, j) for i, j in members] + [L.partner_block(i, j) for i, j in members]

        def pick(n, carry):
            s = block_of(n)
            table = info[s]
            one = jnp.concatenate([picks(table, c).astype(f32) for c in range(4)], axis=0)
            rows = jnp.dot(one.astype(jnp.bfloat16), g[s], preferred_element_type=f32)
            rec[s] = rows.astype(jnp.bfloat16).reshape(4, SLOTS, rows.shape[1])
            return carry

        in_pairs(2 * size, pick)
        middle()

        def score(c, carry):
            rows = jnp.concatenate([rec[k, c] for k in blocks], axis=0)
            out = lax.dot_general(rows, labels[c], (((1,), (1,)), ((), ())), preferred_element_type=f32)
            bias = jnp.sum(rows.astype(f32) * match[c].astype(f32), axis=1, keepdims=True)
            out = out + bias
            for n, k in enumerate(blocks):
                scores[k, c] = out[n * SLOTS : (n + 1) * SLOTS]
            return carry

        lax.fori_loop(0, 4, score, 0)

        def stat(n, carry):
            s = block_of(n)
            table = info[s]
            leaf = lax.broadcasted_iota(jnp.int32, (SLOTS, LEAF), 1).astype(f32)
            parts = []
            for c in range(4):
                one = picks(table, c)
                val = scores[s, c]
                top = jnp.max(val, axis=1, keepdims=True)
                total = jnp.sum(jnp.exp(val - top), axis=1, keepdims=True)
                picked = jnp.sum(
                    jnp.where(leaf == target_column(table, one, c), val, 0.0), axis=1, keepdims=True
                )
                parts.append((one, top, total, picked))
            best = jnp.full((1, table.shape[1]), -BIG, f32)
            for one, top, total, picked in parts:
                best = jnp.maximum(best, jnp.max(jnp.where(one, top, -BIG), axis=0, keepdims=True))
            spread = jnp.zeros_like(best)
            chosen = jnp.zeros_like(best)
            for one, top, total, picked in parts:
                spread += jnp.sum(
                    jnp.where(one, total * jnp.exp(jnp.where(one, top - best, 0.0)), 0.0), axis=0, keepdims=True
                )
                chosen += jnp.sum(jnp.where(one, picked, 0.0), axis=0, keepdims=True)
            st[s] = jnp.concatenate([best, spread, chosen], axis=1)
            return carry

        in_pairs(2 * size, stat)
        for m, k in enumerate(blocks):
            n = base + m
            pltpu.make_async_copy(scores.at[k], scores_out.at[k], out_sem.at[2 * n]).start()
            pltpu.make_async_copy(rec.at[k], rec_out.at[k], out_sem.at[2 * n + 1]).start()
            if n == 0:
                continue
            pltpu.make_async_remote_copy(
                src_ref=st.at[k], dst_ref=sr.at[L.me], send_sem=st_send.at[k], recv_sem=st_recv.at[L.me],
                device_id={"label": k}, device_id_type=MESH,
            ).start()
        return blocks

    side_a(1)
    side_a(2)
    side_b(0)
    order = work(0, far_a)
    far_b(0)
    side_b(1)
    order += work(1, lambda: side_b(2))
    far_b(1)
    side_b(3)
    order += work(2, lambda: far_b(2))
    far_b(3)
    order += work(3, lambda: None)
    sr[own] = st[own]

    def stat_copy(k, arrive):
        return pltpu.make_async_remote_copy(
            src_ref=st.at[k], dst_ref=sr.at[k], send_sem=st_send.at[k], recv_sem=st_recv.at[k],
            device_id={"label": k}, device_id_type=MESH,
        )

    for k in peers:
        stat_copy(k, True).wait_recv()
    q_dev = q_ref.shape[0]
    tops = sr[:, :, 0:q_dev]
    best = jnp.max(tops, axis=0)
    spread = jnp.sum(sr[:, :, q_dev : 2 * q_dev] * jnp.exp(tops - best[None]), axis=0)
    chosen = jnp.sum(sr[:, :, 2 * q_dev : 3 * q_dev], axis=0)
    value = best + jnp.log(spread)
    losses[...] = value - chosen
    lse[own] = value

    def lse_copy(dev, row):
        return pltpu.make_async_remote_copy(
            src_ref=lse.at[row], dst_ref=lse.at[row], send_sem=lse_send.at[dev], recv_sem=lse_recv.at[row],
            device_id={"label": dev}, device_id_type=MESH,
        )

    for k in peers:
        lse_copy(k, own).start()
    for k in peers:
        lse_copy(k, k).wait_recv()
    for k in peers:
        stat_copy(k, False).wait_send()
        lse_copy(k, own).wait_send()
    for n, k in enumerate(order):
        pltpu.make_async_copy(scores.at[k], scores_out.at[k], out_sem.at[2 * n]).wait()
        pltpu.make_async_copy(rec.at[k], rec_out.at[k], out_sem.at[2 * n + 1]).wait()
    L.drain()


def forward(q, labels, match, ids, pos):
    q_dev, width = q.shape
    vmem = pl.BlockSpec(memory_space=pltpu.VMEM)
    hbm = pl.BlockSpec(memory_space=pl.ANY)
    shape = jax.ShapeDtypeStruct
    f32, bf16, dma = jnp.float32, jnp.bfloat16, pltpu.SemaphoreType.DMA
    return pl.pallas_call(
        forward_kernel,
        out_shape=(
            shape((32, 4, SLOTS, LEAF), f32),
            shape((32, 4, SLOTS, width), bf16),
            shape((32, 8, q_dev), f32),
            shape((32, 1, q_dev), f32),
            shape((1, q_dev), f32),
        ),
        in_specs=[vmem] * 5,
        out_specs=(hbm, hbm, vmem, vmem, vmem),
        scratch_shapes=[
            pltpu.VMEM((32, q_dev, width), bf16),
            pltpu.VMEM((32, 4, SLOTS, LEAF), f32),
            pltpu.VMEM((32, 4, SLOTS, width), bf16),
            pltpu.VMEM((32, 1, 3 * q_dev), f32),
            pltpu.VMEM((32, 1, 3 * q_dev), f32),
            dma((36,)), dma((36,)), dma((32,)), dma((32,)), dma((32,)), dma((32,)), dma((64,)),
        ],
        compiler_params=pltpu.CompilerParams(
            collective_id=0, has_side_effects=True, vmem_limit_bytes=60 * 1024 * 1024
        ),
    )(q, labels, match, ids, pos)


class Column:
    def __init__(self, links):
        self.z = lax.axis_index("dp")
        self.links = links

    def copy(self, src, dst, slot, off):
        L = self.links
        n = len(L.sent)
        c = pltpu.make_async_remote_copy(
            src_ref=src, dst_ref=dst, send_sem=L.send.at[n], recv_sem=L.recv.at[slot],
            device_id={"dp": lax.rem(self.z + off, 4)}, device_id_type=MESH,
        )
        c.start()
        L.sent.append(c)


BACK_TURNS = (
    ((3, 3), (1, 3), (2, 3), (0, 3)),
    ((3, 1), (3, 2), (1, 1), (1, 2)),
    ((2, 1), (2, 2), (0, 1), (0, 2)),
    ((3, 0), (1, 0), (2, 0), (0, 0)),
)


def backward_kernel(labels, match, info, lse, scores_hbm, rec_hbm, out, label_out, mout,
                    stage, rec, delta, coef, grads, p, lp, ls, pr, bh, bf, ah, af, zh, zf, mz,
                    send, recv, m_recv, in_sem):
    L = Links(send, recv)
    Z = Column(L)
    z = Z.z
    f32, bf16 = jnp.float32, jnp.bfloat16
    turns = [
        [L.block(i, j) for i, j in t] + [L.partner_block(i, j) for i, j in t] for t in BACK_TURNS
    ]

    def load_scores(t):
        return [
            pltpu.make_async_copy(scores_hbm.at[k], stage.at[t % 2, m], in_sem.at[0, 8 * t + m])
            for m, k in enumerate(turns[t])
        ]

    def load_rows(t):
        return [
            pltpu.make_async_copy(rec_hbm.at[k], rec.at[k], in_sem.at[1, 8 * t + m])
            for m, k in enumerate(turns[t])
        ]

    for t in range(2):
        for c in load_scores(t) + load_rows(t):
            c.start()
    for t in range(2, 4):
        for c in load_rows(t):
            c.start()
    peers = [L.block(i, j) for i in range(4) for j in range(4)][1:]
    peers += [L.partner_block(i, j) for i in range(4) for j in range(4)]
    barrier = pltpu.get_barrier_semaphore()
    for d in peers:
        pl.semaphore_signal(barrier, inc=1, device_id={"label": d}, device_id_type=MESH)
    for off in (1, 2, 3):
        pl.semaphore_signal(barrier, inc=1, device_id={"dp": lax.rem(z + off, 4)}, device_id_type=MESH)
    ls[...] = jnp.zeros_like(ls)

    def block_of(t, n):
        code_a = sum(OFF[i] << (2 * m) for m, (i, j) in enumerate(BACK_TURNS[t]))
        code_b = sum(OFF[j] << (2 * m) for m, (i, j) in enumerate(BACK_TURNS[t]))
        other, m = n // 4, lax.rem(n, 4)
        core = L.core + other - 2 * L.core * other
        da = lax.rem(lax.shift_right_logical(jnp.int32(code_a), 2 * m), 4)
        db = lax.rem(lax.shift_right_logical(jnp.int32(code_b), 2 * m), 4)
        a = lax.rem(L.a * (1 - other) + L.b * other + da, 4)
        b = lax.rem(L.b * (1 - other) + L.a * other + db, 4)
        return index_of(core, a, b)

    def part(t):
        for c in load_scores(t) + load_rows(t):
            c.wait()

        def step(n, carry):
            k = block_of(t, n)
            table = info[k]
            leaf = lax.broadcasted_iota(jnp.int32, (SLOTS, LEAF), 1).astype(f32)
            log_sum = lse[k]
            for c in range(4):
                one = picks(table, c)
                used = jnp.sum(jnp.where(one, 1.0, 0.0), axis=1, keepdims=True) > 0.5
                norm = jnp.sum(jnp.where(one, log_sum, 0.0), axis=1, keepdims=True)
                norm = jnp.where(used, norm, BIG)
                hit = leaf == target_column(table, one, c)
                value = jnp.exp(stage[t % 2, n, c] - norm) - hit.astype(f32)
                total = jnp.sum(value, axis=1, keepdims=True).astype(bf16)
                delta[k, c] = value.astype(bf16)
                coef[k, c] = jnp.broadcast_to(total.astype(f32), (SLOTS, 128)).astype(bf16)
                ls[c] += jnp.sum(total.astype(f32) * rec[k, c].astype(f32), axis=0, keepdims=True)
            return carry

        in_pairs(8, step)
        if t < 2:
            for c in load_scores(t + 2):
                c.start()

    def slots(t):
        def slot(c, carry):
            rows = jnp.concatenate([delta[k, c] for k in turns[t]], axis=0)
            scale = jnp.concatenate([coef[k, c] for k in turns[t]], axis=0)[:, 0:1].astype(f32)
            val = jnp.dot(rows, labels[c], preferred_element_type=f32)
            val = (val + scale * match[c].astype(f32)).astype(bf16)
            for n in range(8):
                grads[n, pl.ds(pl.multiple_of(c * SLOTS, 16), SLOTS)] = val[n * SLOTS : (n + 1) * SLOTS]
            return carry

        lax.fori_loop(0, 4, slot, 0)

        def back(n, carry):
            k = block_of(t, n)
            table = info[k]
            one = jnp.concatenate([picks(table, c).astype(f32) for c in range(4)], axis=0).astype(bf16)
            val = lax.dot_general(one, grads[n], (((0,), (0,)), ((), ())), preferred_element_type=f32)
            p[k] = val.astype(bf16)
            return carry

        in_pairs(8, back)
        for i, j in BACK_TURNS[t]:
            L.copy(p.at[L.partner_block(i, j)], pr.at[4 * i + j], 4 * i + j, "p")

    def label_parts(low):
        def one_part(c, carry):
            left = jnp.concatenate([delta[k, c] for k in range(32)], axis=0)
            right = jnp.concatenate([rec[k, c] for k in range(32)], axis=0)
            val = lax.dot_general(left, right, (((0,), (0,)), ((), ())), preferred_element_type=f32)
            lp[c] = val.astype(bf16)
            return carry

        lax.fori_loop(low, low + 2, one_part, 0)

    half = p.shape[1] // 2
    rows_z = label_out.shape[1]

    def rows(off):
        return pl.ds(pl.multiple_of(lax.rem(z + off, 4) * rows_z, rows_z), rows_z)

    PAIRS = pl.ds(0, 2), pl.ds(2, 2)
    LO, HI = pl.ds(0, half), pl.ds(half, half)

    def both(i, j):
        L.wait(pr.at[4 * i + j], 4 * i + j)
        return lambda s: p[L.block(i, j), s].astype(f32) + pr[4 * i + j, s].astype(f32)

    def far(i):
        s = both(i, 3)
        t = p.at[L.block(i, 3)]
        t[...] = s(slice(None)).astype(t.dtype)
        L.copy(t.at[LO], bh.at[i, 0], 16 + 4 * i, "b+")
        L.copy(t.at[HI], bh.at[i, 1], 17 + 4 * i, "b-")

    def near(i):
        s = both(i, 2)
        t = p.at[L.block(i, 2)]
        L.wait(bh.at[i, 0], 16 + 4 * i)
        t[LO] = (s(LO) + bh[i, 0].astype(f32)).astype(t.dtype)
        t[HI] = s(HI).astype(t.dtype)
        L.copy(t, bf.at[i, 0], 18 + 4 * i, "b+")
        s = both(i, 1)
        t = p.at[L.block(i, 1)]
        L.wait(bh.at[i, 1], 17 + 4 * i)
        t[HI] = (s(HI) + bh[i, 1].astype(f32)).astype(t.dtype)
        t[LO] = s(LO).astype(t.dtype)
        L.copy(t, bf.at[i, 1], 19 + 4 * i, "b-")

    def column(i):
        s = both(i, 0)
        L.wait(bf.at[i, 0], 18 + 4 * i)
        L.wait(bf.at[i, 1], 19 + 4 * i)
        return lambda r: s(r) + bf[i, 0, r].astype(f32) + bf[i, 1, r].astype(f32)

    def row_copy(dev, row):
        return pltpu.make_async_remote_copy(
            src_ref=mout.at[z, row], dst_ref=mout.at[z, row], send_sem=m_recv.at[1, dev], recv_sem=m_recv.at[0, row],
            device_id={"label": dev}, device_id_type=MESH,
        )

    part(0)
    pl.semaphore_wait(barrier, 34)
    slots(0)
    part(1)
    for i in (3, 1, 2, 0):
        far(i)
    part(2)
    part(3)
    mz[z] = ls[z]
    for off in (1, 2, 3):
        Z.copy(ls.at[lax.rem(z + off, 4)], mz.at[z], 41 + off, off)
    slots(1)
    label_parts(0)
    Z.copy(lp.at[PAIRS[0], rows(2)], zh.at[0], 36, 1)
    near(3)
    near(1)
    label_parts(2)
    Z.copy(lp.at[PAIRS[1], rows(2)], zh.at[1], 37, 3)
    for off in (1, 2, 3):
        L.wait(mz.at[lax.rem(z + 4 - off, 4)], 41 + off)
    mout[z, L.me] = mz[0] + mz[1] + mz[2] + mz[3]
    for k in peers:
        row_copy(k, L.me).start()
    slots(2)
    L.wait(zh.at[0], 36)
    lp[PAIRS[0], rows(1)] = (lp[PAIRS[0], rows(1)].astype(f32) + zh[0].astype(f32)).astype(bf16)
    Z.copy(lp.at[:, rows(1)], zf.at[0], 38, 1)
    near(2)
    near(0)
    L.wait(zh.at[1], 37)
    lp[PAIRS[1], rows(3)] = (lp[PAIRS[1], rows(3)].astype(f32) + zh[1].astype(f32)).astype(bf16)
    Z.copy(lp.at[:, rows(3)], zf.at[1], 39, 3)
    slots(3)
    for k in peers:
        row_copy(k, k).wait_recv()
    for off in (1, 2, 3):
        Z.copy(mout.at[z], mout.at[z], 44 + off, off)
    s = column(3)
    u = p.at[L.block(3, 0)]
    u[...] = s(slice(None)).astype(u.dtype)
    L.copy(u.at[LO], ah.at[0], 32, "a+")
    L.copy(u.at[HI], ah.at[1], 33, "a-")
    s = column(1)
    u = p.at[L.block(1, 0)]
    L.wait(ah.at[1], 33)
    u[HI] = (s(HI) + ah[1].astype(f32)).astype(u.dtype)
    u[LO] = s(LO).astype(u.dtype)
    L.copy(u, af.at[1], 35, "a-")
    s = column(2)
    u = p.at[L.block(2, 0)]
    L.wait(ah.at[0], 32)
    u[LO] = (s(LO) + ah[0].astype(f32)).astype(u.dtype)
    u[HI] = s(HI).astype(u.dtype)
    L.copy(u, af.at[0], 34, "a+")
    L.wait(zf.at[0], 38)
    L.wait(zf.at[1], 39)
    label_out[...] = lp[:, rows(0)].astype(f32) + zf[0].astype(f32) + zf[1].astype(f32)
    s = column(0)
    L.wait(af.at[0], 34)
    L.wait(af.at[1], 35)
    out[...] = s(slice(None)) + af[0].astype(f32) + af[1].astype(f32)
    for off in (1, 2, 3):
        L.wait(mout.at[lax.rem(z + 4 - off, 4)], 44 + off)
    for k in peers:
        row_copy(k, L.me).wait_send()
    L.drain()


def backward(labels, match, info, lse, scores, rec):
    n, _, r = info.shape
    clusters, leaf, w = labels.shape
    f32, bf16, dma = jnp.float32, jnp.bfloat16, pltpu.SemaphoreType.DMA
    vmem = pl.BlockSpec(memory_space=pltpu.VMEM)
    hbm = pl.BlockSpec(memory_space=pl.ANY)
    shape = jax.ShapeDtypeStruct
    return pl.pallas_call(
        backward_kernel,
        out_shape=(shape((r, w), f32), shape((clusters, leaf // 4, w), f32), shape((4, n, 1, w), f32)),
        in_specs=[vmem] * 4 + [hbm] * 2,
        out_specs=(vmem,) * 3,
        scratch_shapes=[
            pltpu.VMEM((2, 8, 4, SLOTS, leaf), f32),
            pltpu.VMEM((n, 4, SLOTS, w), bf16),
            pltpu.VMEM((n, 4, SLOTS, leaf), bf16),
            pltpu.VMEM((n, 4, SLOTS, 128), bf16),
            pltpu.VMEM((8, 4 * SLOTS, w), bf16),
            pltpu.VMEM((n, r, w), bf16),
            pltpu.VMEM((clusters, leaf, w), bf16),
            pltpu.VMEM((clusters, 1, w), f32),
            pltpu.VMEM((16, r, w), bf16),
            pltpu.VMEM((4, 2, r // 2, w), bf16),
            pltpu.VMEM((4, 2, r, w), bf16),
            pltpu.VMEM((2, r // 2, w), bf16),
            pltpu.VMEM((2, r, w), bf16),
            pltpu.VMEM((2, 2, leaf // 4, w), bf16),
            pltpu.VMEM((2, clusters, leaf // 4, w), bf16),
            pltpu.VMEM((4, 1, w), f32),
            dma((52,)),
            dma((48,)),
            dma((2, 32)),
            dma((2, 32)),
        ],
        compiler_params=pltpu.CompilerParams(
            collective_id=1, has_side_effects=True, vmem_limit_bytes=67043328
        ),
    )(labels, match, info, lse, scores, rec)


def body(queries, labels, matcher, cluster_ids, positives):
    q_dev, width = queries.shape
    cl_dev = labels.shape[0]
    n_label = lax.axis_size("label")
    first = lax.axis_index("label") * cl_dev
    match = lax.dynamic_slice_in_dim(matcher, first, cl_dev, 0).reshape(cl_dev, 1, width)
    ids = cluster_ids.reshape(n_label, q_dev, K).transpose(0, 2, 1)
    pos = positives.reshape(n_label, 1, q_dev)
    scores, received, info, lse, losses = forward(queries, labels, match, ids, pos)
    query_grads, label_grads, rows = backward(labels, match, info, lse, scores, received)
    matcher_grads = rows.transpose(1, 0, 2, 3).reshape(matcher.shape)
    return (losses.reshape(q_dev), query_grads, label_grads, matcher_grads)


def solution(mesh):
    return jax.shard_map(
        body,
        mesh=mesh,
        in_specs=(P(("dp", "label"), None), P("label", None, None), P(), P("dp", None), P("dp")),
        out_specs=(P(("dp", "label")), P(("dp", "label"), None), P("label", "dp", None), P()),
        check_vma=False,
    )
```
